256 devices in a mesh: prow: 8 (over x_lo, y), pcol: 32 (over z, x_hi, core).
Axes of the slice: x: 4 (x_hi: 2, x_lo: 2; x = x_hi * 2 + x_lo), y: 4, z: 8, core: 2. Of those that a mesh axis runs over, the one named last changes fastest.
Arguments:
- inverse_factor: float32 [1024, 1024], P('pcol'), as said below
- diag_block: float32 [1024, 1024], P('pcol'), as said below
- panel_matrix: float32 [16, 8, 128, 1024], P(None, 'prow', 'pcol'), may hold values from -6 to 6
- panel_factor: float32 [16, 8, 128, 1024], P(None, 'prow', 'pcol'), may hold values from -0.1875 to 0.1875
- trailing: float32 [16, 8, 128, 4, 32, 128], P(None, 'prow', None, None, 'pcol'), may hold values from -6 to 6
Outputs:
- reduced_diag: float32 [1024, 1024], P('pcol')
- panel_result: float32 [16, 8, 128, 1024], P(None, 'prow', 'pcol')
- trailing_out: float32 [16, 8, 128, 4, 32, 128], P(None, 'prow', None, None, 'pcol')
The draws below stay inside these ranges and needn't reach their ends.
Inputs may be any that keep to these rules, and one draw needn't show every extreme that they name: `inverse_factor`: lower triangular, diagonal entries between 0.5 and 2. `diag_block`: symmetric.
All inputs are finite; a program needn't handle non-finite values.
Results may differ from the reference program's by a relative error of at most 0.0003.
Values sent between devices are 32-bit elements; how exact they have to be, the bound alone decides.
A program may use at most 128 MiB of HBM per device.

```python
import jax
import jax.numpy as jnp
from jax import lax

NB = 1024
TILE = 128
MR = 16
M = 16384
MC = 4
N_PROW = 8
N_PCOL = 32


def draw_inverse_factor(key, part):
    first, second = jax.random.split(jax.random.fold_in(key, 11), 2)
    spread = jax.random.normal(first, (NB, NB), jnp.float32) * (0.6 / NB ** 0.5)
    diagonal = jnp.exp(jax.random.uniform(second, (NB,), jnp.float32, -0.69, 0.69))
    return jnp.tril(spread, -1) + jnp.diag(diagonal)


def draw_diag_block(key, part):
    first = jax.random.fold_in(key, 23)
    base = jax.random.normal(first, (NB, NB), jnp.float32)
    return (base + base.T) * 0.70710678


def block_levels(stream_key, extent, cuts, low, largest):
    loudness = 1.0
    for axis_at, parts in cuts:
        steps = jax.random.uniform(jax.random.fold_in(jax.random.fold_in(stream_key, 6), axis_at), (parts,), jnp.float32, low / len(cuts), largest / len(cuts))
        loudness = loudness * jnp.repeat(jnp.exp(steps), extent[axis_at] // parts).reshape((-1,) + (1,) * (len(extent) - 1 - axis_at))
    return loudness


def centred(stream_key, extent, scale, most, pieces=(), held_as=jnp.bfloat16):
    entries = scale * jax.random.normal(stream_key, extent, jnp.float32)
    if pieces:
        entries = entries * block_levels(stream_key, extent, pieces, -0.22, 0.18)
    return jnp.clip(entries, -most, most).astype(held_as)


def setup_inputs(seed: int = 0) -> dict:
    keys = jax.random.split(jax.random.key(seed), 6)
    return {
        "inverse_factor": draw_inverse_factor(jax.random.fold_in(keys[5], 71), 0),
        "diag_block": draw_diag_block(jax.random.fold_in(keys[5], 71), 0),
        "panel_matrix": centred(keys[2], (MR, N_PROW, TILE, NB), 1.0, 6.0, ((1, 8), (2, 32)), jnp.float32),
        "panel_factor": centred(keys[3], (MR, N_PROW, TILE, NB), NB ** -0.5, 0.1875, ((1, 8), (2, 32)), jnp.float32),
        "trailing": centred(keys[4], (MR, N_PROW, TILE, MC, N_PCOL, TILE), 1.0, 6.0, ((1, 8), (4, 32)), jnp.float32),
    }


def reference(inverse_factor, diag_block, panel_matrix, panel_factor, trailing):
    exact = lax.Precision.HIGHEST
    order = M
    inner = jnp.dot(diag_block, inverse_factor.T, precision=exact, preferred_element_type=jnp.float32)
    reduced = jnp.dot(inverse_factor, inner, precision=exact, preferred_element_type=jnp.float32)
    panel = panel_matrix.reshape(order, NB)
    factor = panel_factor.reshape(order, NB)
    solved = jnp.dot(panel, inverse_factor.T, precision=exact, preferred_element_type=jnp.float32)
    coupled = jnp.dot(factor, reduced, precision=exact, preferred_element_type=jnp.float32)
    shifted = solved - 0.5 * coupled
    result = shifted - 0.5 * coupled
    whole = trailing.reshape(order, order)
    col_tile = jnp.arange(order, dtype=jnp.int32) // TILE

    def one_row(index):
        start = (index * TILE).astype(jnp.int32)
        rows_a = lax.dynamic_slice_in_dim(whole, start, TILE, 0)
        rows_y = lax.dynamic_slice_in_dim(shifted, start, TILE, 0)
        rows_f = lax.dynamic_slice_in_dim(factor, start, TILE, 0)
        update = jnp.dot(rows_y, factor.T, precision=exact, preferred_element_type=jnp.float32)
        update = update + jnp.dot(rows_f, shifted.T, precision=exact, preferred_element_type=jnp.float32)
        return jnp.where(col_tile[None, :] <= index, rows_a - update, rows_a)

    blocks = lax.map(one_row, jnp.arange(order // TILE, dtype=jnp.int32))
    trailing_out = blocks.reshape(trailing.shape)
    return reduced, result.reshape(panel_matrix.shape), trailing_out
```

```python
import functools

import jax
import jax.numpy as jnp
from jax import lax
from jax.experimental import pallas as pl
from jax.experimental.pallas import tpu as pltpu
from jax.sharding import PartitionSpec as P

MESH = pl.DeviceIdType.MESH
F32 = jnp.float32
BF16 = jnp.bfloat16


def comm_kernel(own, oth, eown, eoth, g_ref, cm_ref, cp_ref, h_ref,
                merged, swap, loc_sem, pre_send, pre_recv, xh_send, xh_recv,
                z_send, z_recv, d_send, d_recv, c_send, c_recv, cd_send, cd_recv,
                e_pre, ez_send, ez_recv, ey_send, ey_recv, ed_send, ed_recv):
    a = lax.axis_index("prow")
    c = lax.axis_index("pcol")
    xl, y = a // 4, a % 4
    z, xh, k = c // 4, (c // 2) % 2, c % 2
    d = c // 2

    partner = (a, c + 1 - 2 * k)
    z_next = (a, ((z + 1) % 8) * 4 + xh * 2 + k)
    z_prev = (a, ((z + 7) % 8) * 4 + xh * 2 + k)
    x_far = (a, z * 4 + (1 - xh) * 2 + k)
    x_near = ((1 - xl) * 4 + y, c)
    y_next = (xl * 4 + (y + 1) % 4, c)
    y_prev = (xl * 4 + (y + 3) % 4, c)
    z_to = (z_next, z_prev)

    def remote(src, dst, send, recv, to):
        return pltpu.make_async_remote_copy(
            src_ref=src, dst_ref=dst, send_sem=send, recv_sem=recv, device_id=to, device_id_type=MESH
        )

    barrier = pltpu.get_barrier_semaphore()
    for to in (partner, z_next, z_prev, x_far, x_near, y_next, y_prev):
        pl.semaphore_signal(barrier, inc=1, device_id=to, device_id_type=MESH)
    pl.semaphore_wait(barrier, 7)

    def h_rows(which, block, start, size):
        return h_ref.at[which, block, pl.ds(pl.multiple_of(start, 32), size), :]

    pre_e = remote(eoth, h_rows(1 - k, a, 32 * c, 32), e_pre.at[0], e_pre.at[1], partner)
    pre_e.start()
    pre = remote(oth, swap, pre_send, pre_recv, partner)
    pre.start()
    mine_e = pltpu.make_async_copy(eown, h_rows(k, a, 32 * c, 32), e_pre.at[2])
    mine_e.start()

    mine_e.wait()
    remote(eoth, h_rows(k, a, 32 * (c + 1 - 2 * k), 32), e_pre.at[0], e_pre.at[1], partner).wait_recv()
    far_e = remote(h_rows(k, a, 64 * d, 64), h_rows(k, a, 64 * d, 64), e_pre.at[3], e_pre.at[4], x_far)
    far_e.start()

    pre.wait_recv()
    merged[...] = own[...] + swap[...]

    def g_rows(which, j, n, start, size):
        return g_ref.at[which, pl.ds(j, n), :, pl.ds(pl.multiple_of(start, 8), size), :]

    far = remote(merged, g_ref.at[k, :, :, pl.ds(pl.multiple_of(8 * d, 8), 8), :], xh_send, xh_recv, x_far)
    far.start()
    mine = pltpu.make_async_copy(merged, g_ref.at[k, :, :, pl.ds(pl.multiple_of(8 * d, 8), 8), :], loc_sem)
    mine.start()

    df = 2 * z + 1 - xh
    remote(
        h_rows(k, a, 64 * df, 64), h_rows(k, a, 64 * df, 64), e_pre.at[3], e_pre.at[4], x_far
    ).wait_recv()

    def ez_copy(h, t):
        at = (z + 8 - t) % 8 if h == 0 else (z + t) % 8
        ref = h_rows(k, a, 128 * at, 128)
        return remote(ref, ref, ez_send.at[h, t], ez_recv.at[h, t], z_to[h])

    def ez_got(h, t):
        at = (z + 8 - t) % 8 if h == 0 else (z + t) % 8
        ref = h_rows(k, a, 128 * at, 128)
        return remote(ref, ref, ez_send.at[h, t - 1], ez_recv.at[h, t - 1], z_to[h])

    for h in range(2):
        ez_copy(h, 0).start()
    for t in range(1, 5):
        for h in range(2):
            if t <= (4, 3)[h]:
                ez_got(h, t).wait_recv()
                if t < (4, 3)[h]:
                    ez_copy(h, t).start()

    def plane(h, t):
        return lax.rem(z + 8 - t, 8) if h == 0 else lax.rem(z + t, 8)

    def z_ref(h, t, e):
        side = xh if e == 0 else 1 - xh
        return g_rows(k, 2 * h, 2, 16 * plane(h, t) + 8 * side, 8)

    def z_copy(h, t, e):
        ref = z_ref(h, t, e)
        return remote(ref, ref, z_send.at[h, e, t], z_recv.at[h, e, t], z_to[h])

    def z_got(h, t, e):
        ref = z_ref(h, t, e)
        return remote(ref, ref, z_send.at[h, e, t - 1], z_recv.at[h, e, t - 1], z_to[h])

    def d_copy(h, t, which=None):
        ref = g_rows(k if which is None else which, 2 * h, 2, 16 * plane(h, t), 16)
        return remote(ref, ref, d_send.at[h, t], d_recv.at[h, t], partner)

    mine.wait()
    for h in range(2):
        z_copy(h, 0, 0).start()

    def e_block(dx, dy):
        return (xl + dx) % 2 * 4 + (y + dy) % 4

    def e_copy(dx, dy, to, rdx, rdy, out):
        ref = h_ref.at[k, e_block(dx, dy)]
        return remote(ref, ref, ey_send.at[out], ey_recv.at[rdx * 4 + rdy], to)

    def e_got(dx, dy):
        ref = h_ref.at[k, e_block(dx, dy)]
        return remote(ref, ref, ey_send.at[0], ey_recv.at[dx * 4 + dy], partner)

    def e_pass(dx, dy, which=None):
        ref = h_ref.at[k if which is None else which, e_block(dx, dy)]
        return remote(ref, ref, ed_send.at[dx * 4 + dy], ed_recv.at[dx * 4 + dy], partner)

    e_sends = [
        e_copy(0, 0, x_near, 1, 0, 0),
        e_copy(0, 0, y_next, 0, 3, 1),
        e_copy(0, 0, y_prev, 0, 1, 2),
        e_copy(1, 0, y_next, 1, 3, 3),
        e_copy(1, 0, y_prev, 1, 1, 4),
        e_copy(0, 1, y_prev, 0, 2, 5),
        e_copy(1, 3, y_next, 1, 2, 6),
    ]
    for n in range(3):
        e_sends[n].start()
    e_pass(0, 0).start()

    remote(
        merged, g_ref.at[k, :, :, pl.ds(pl.multiple_of(8 * df, 8), 8), :], xh_send, xh_recv, x_far
    ).wait_recv()
    for h in range(2):
        z_copy(h, 0, 1).start()
        d_copy(h, 0).start()

    q = z // 2
    in_plane = xl == z % 2

    def place(m):
        return lax.rem(y - (2 * xh + m) + 4, 4)

    def c_ref(m, h, t):
        return cm_ref.at[m, pl.ds(2 * h, 2), pl.ds(pl.multiple_of(16 * plane(h, t), 16), 16), :]

    def c_copy(m, h, t, out, from_g):
        dst = c_ref(m, h, t)
        src = (
            g_ref.at[k, pl.ds(2 * h, 2), q, pl.ds(pl.multiple_of(16 * plane(h, t), 16), 16), :]
            if from_g
            else dst
        )
        to = (x_near, y_next, y_prev)[out]
        return remote(src, dst, c_send.at[m, h, t, out], c_recv.at[m, h, t], to)

    def cd_copy(m, h, t):
        dst = cp_ref.at[pl.ds(2 * h, 2), pl.ds(pl.multiple_of(16 * plane(h, t), 16), 16), :]
        return remote(c_ref(m, h, t), dst, cd_send.at[h, t], cd_recv.at[h, t], partner)

    def each_send(m, h, t, act):
        r = place(m)

        @pl.when(jnp.logical_and(in_plane, r == 0))
        def _():
            for out in range(3):
                act(c_copy(m, h, t, out, True))

        @pl.when(jnp.logical_and(jnp.logical_not(in_plane), r == 0))
        def _():
            for out in (1, 2):
                act(c_copy(m, h, t, out, False))

        @pl.when(r == (3 if m == 0 else 1))
        def _():
            act(c_copy(m, h, t, 2 if m == 0 else 1, False))

    def source_sends(t):
        for m in range(2):
            @pl.when(jnp.logical_and(in_plane, place(m) == 0))
            def _():
                for h in range(2):
                    for out in range(3):
                        c_copy(m, h, t, out, True).start()

    def take_columns(t, when):
        for m in range(2):
            r = place(m)
            got = jnp.logical_not(jnp.logical_and(in_plane, r == 0))
            early = jnp.logical_or(r == 0, jnp.logical_and(in_plane, r != 2))

            @pl.when(jnp.logical_and(got, early if when else jnp.logical_not(early)))
            def _():
                for h in range(2):
                    c_copy(m, h, t, 0, False).wait_recv()

                    @pl.when(r == 0)
                    def _():
                        for out in (1, 2):
                            c_copy(m, h, t, out, False).start()

                    @pl.when(r == (3 if m == 0 else 1))
                    def _():
                        c_copy(m, h, t, 2 if m == 0 else 1, False).start()

                    @pl.when(k != m)
                    def _():
                        cd_copy(m, h, t).start()

    source_sends(0)

    def step(t, carry):
        for e in range(2):
            for h in range(2):
                z_got(h, t, e).wait_recv()

                @pl.when(t < 7)
                def _():
                    z_copy(h, t, e).start()

        for h in range(2):
            d_copy(h, t).start()
        source_sends(t)
        take_columns(t - 1, True)

        @pl.when(t >= 2)
        def _():
            take_columns(t - 2, False)

        @pl.when(t == 1)
        def _():
            e_got(1, 0).wait_recv()
            e_sends[3].start()
            e_sends[4].start()
            e_pass(1, 0).start()

        @pl.when(t == 3)
        def _():
            e_got(0, 1).wait_recv()
            e_sends[5].start()
            e_pass(0, 1).start()
            e_got(0, 3).wait_recv()
            e_pass(0, 3).start()

        @pl.when(t == 4)
        def _():
            e_got(1, 3).wait_recv()
            e_sends[6].start()
            e_pass(1, 3).start()
            e_got(1, 1).wait_recv()
            e_pass(1, 1).start()

        @pl.when(t == 6)
        def _():
            for dx in range(2):
                e_got(dx, 2).wait_recv()
                e_pass(dx, 2).start()

        return carry

    lax.fori_loop(1, 8, step, 0)
    take_columns(7, True)
    take_columns(6, False)
    take_columns(7, False)

    pre_e.wait_send()
    pre.wait_send()
    far_e.wait_send()
    far.wait_send()
    for h in range(2):
        for t in range((4, 3)[h]):
            ez_copy(h, t).wait_send()
    for n in range(7):
        e_sends[n].wait_send()
    for dx in range(2):
        for dy in range(4):
            e_pass(dx, dy).wait_send()
            e_pass(dx, dy, 1 - k).wait_recv()

    def finish(t, carry):
        for h in range(2):
            @pl.when(t < 7)
            def _():
                for e in range(2):
                    z_copy(h, t, e).wait_send()

            d_copy(h, t).wait_send()
            d_copy(h, t, 1 - k).wait_recv()
            for m in range(2):
                each_send(m, h, t, lambda copy: copy.wait_send())
                source = jnp.logical_and(in_plane, place(m) == 0)

                @pl.when(jnp.logical_not(source))
                def _():
                    @pl.when(k != m)
                    def _():
                        cd_copy(m, h, t).wait_send()

                    @pl.when(k == m)
                    def _():
                        cd_copy(m, h, t).wait_recv()

        return carry

    lax.fori_loop(0, 8, finish, 0)


def gather(own, oth, eown, eoth):
    dma = pltpu.SemaphoreType.DMA
    return pl.pallas_call(
        comm_kernel,
        out_shape=(
            jax.ShapeDtypeStruct((2, 4, 4, 128, 1024), F32),
            jax.ShapeDtypeStruct((2, 4, 128, 1024), F32),
            jax.ShapeDtypeStruct((4, 128, 1024), F32),
            jax.ShapeDtypeStruct((2, 8, 1024, 128), F32),
        ),
        in_specs=[pl.BlockSpec(memory_space=pltpu.VMEM)] * 4,
        out_specs=(pl.BlockSpec(memory_space=pl.ANY),) * 4,
        scratch_shapes=[
            pltpu.VMEM((4, 4, 8, 1024), F32),
            pltpu.VMEM((4, 4, 8, 1024), F32),
            dma, dma, dma, dma, dma,
            dma((2, 2, 7)), dma((2, 2, 7)),
            dma((2, 8)), dma((2, 8)),
            dma((2, 2, 8, 3)), dma((2, 2, 8)),
            dma((2, 8)), dma((2, 8)),
            dma((5,)),
            dma((2, 4)), dma((2, 4)),
            dma((7,)), dma((8,)),
            dma((8,)), dma((8,)),
        ],
        compiler_params=pltpu.CompilerParams(collective_id=0, has_side_effects=True),
        name="gather",
    )(own, oth, eown, eoth)


def split(v):
    hi = v.astype(BF16)
    return hi, (v - hi.astype(F32)).astype(BF16)


def dot3(x, y, contract):
    (xh, xlo), (yh, ylo) = x, y
    dims = (((1,), (contract,)), ((), ()))
    dot = functools.partial(lax.dot_general, dimension_numbers=dims, preferred_element_type=F32)
    return dot(xh, yh) + dot(xlo, yh) + dot(xh, ylo)


ROWS = 608


def update_kernel(pb, fb, tr, g_ref, cm_ref, cp_ref, h_ref, pown, fown, iown,
                  red_ref, panel_ref, out_ref,
                  pc, fc, hv, ih, il, dh, dl, uh, ul, th, tl, vh, vl, sems):
    b = pl.program_id(0)
    a = lax.axis_index("prow")
    c = lax.axis_index("pcol")
    z, xh, k = c // 4, (c // 2) % 2, c % 2
    source = a == (z % 2) * 4 + 2 * xh + k

    @pl.when(b == 0)
    def _():
        load_h = pltpu.make_async_copy(h_ref, hv, sems.at[2])
        load_h.start()

        @pl.when(source)
        def _():
            pltpu.make_async_copy(g_ref.at[0, :, z // 2], pc, sems.at[0]).start()
            pltpu.make_async_copy(g_ref.at[1, :, z // 2], fc, sems.at[1]).start()

        @pl.when(jnp.logical_not(source))
        def _():
            @pl.when(k == 0)
            def _():
                pltpu.make_async_copy(cm_ref.at[0], pc, sems.at[0]).start()
                pltpu.make_async_copy(cp_ref, fc, sems.at[1]).start()

            @pl.when(k == 1)
            def _():
                pltpu.make_async_copy(cp_ref, pc, sems.at[0]).start()
                pltpu.make_async_copy(cm_ref.at[1], fc, sems.at[1]).start()

        load_h.wait()
        for g in range(8):
            lanes = slice(128 * g, 128 * g + 128)
            hi, lo = split(hv[0, g])
            ih[:, lanes] = hi
            il[:, lanes] = lo
            hi, lo = split(hv[1, g])
            dh[:, lanes] = hi
            dl[:, lanes] = lo
        pltpu.make_async_copy(cm_ref.at[0], pc, sems.at[0]).wait()
        pltpu.make_async_copy(cm_ref.at[0], fc, sems.at[1]).wait()

        hi, lo = split(fc[...].reshape(512, 1024))
        th[0:512] = hi
        tl[0:512] = lo
        hi, lo = split(fown[...])
        th[512:576] = hi
        tl[512:576] = lo
        for n in range(4):
            cols = slice(256 * n, 256 * n + 256)
            deep = slice(256 * n, 1024)
            u = dot3(
                (th[0:576, deep], tl[0:576, deep]), (ih[deep, cols], il[deep, cols]), 0
            )
            hi, lo = split(u)
            uh[0:576, cols] = hi
            ul[0:576, cols] = lo
        hi, lo = split(iown[...])
        uh[576:608] = hi
        ul[576:608] = lo
        for n in range(4):
            cols = slice(256 * n, 256 * n + 256)
            start = jnp.concatenate(
                [pc[:, :, cols].reshape(512, 256), pown[:, cols], jnp.zeros((32, 256), F32)]
            )
            t = start - dot3((uh[...], ul[...]), (dh[:, cols], dl[:, cols]), 0)
            hi, lo = split(t)
            th[:, cols] = hi
            tl[:, cols] = lo
        for n in range(4):
            cols = slice(256 * n, 256 * n + 256)
            deep = slice(0, 256 * n + 256)
            v = dot3((th[:, deep], tl[:, deep]), (ih[cols, deep], il[cols, deep]), 1)
            hi, lo = split(v[0:512])
            vh[:, cols] = hi
            vl[:, cols] = lo
            panel_ref[:, cols] = v[512:576]
            red_ref[:, cols] = -v[576:608]

    for n in range(4):
        @pl.when(b == n)
        def _():
            wide = slice(0, 128 * n + 128)
            for q in range(2):
                first = split(pb[0, 0, 2 * q:2 * q + 2].reshape(256, 1024))
                second = split(fb[0, 0, 2 * q:2 * q + 2].reshape(256, 1024))
                total = dot3(first, (uh[wide], ul[wide]), 1) + dot3(second, (vh[wide], vl[wide]), 1)
                for p in range(2):
                    i = 2 * q + p
                    lower = 8 * i + a >= c
                    for j in range(4):
                        at = pl.ds(j, 128, stride=4)
                        held = tr[i, at, :]
                        if j <= n:
                            new = held - total[128 * p:128 * p + 128, 128 * j:128 * j + 128]
                            held = jnp.where(lower, new, held) if j == n else new
                        out_ref[i, at, :] = held


def update(g, cm, cp, hh, pown, fown, iown, trailing):
    any_ = pl.BlockSpec(memory_space=pl.ANY)
    fixed = lambda shape: pl.BlockSpec(shape, lambda b: (0,) * len(shape), pipeline_mode=pl.Buffered(1))
    half = lambda which: pl.BlockSpec((1, 1, 4, 128, 1024), lambda b: (which, b, 0, 0, 0))
    tiles = pl.BlockSpec((4, 512, 128), lambda b: (b, 0, 0))
    return pl.pallas_call(
        update_kernel,
        grid=(4,),
        out_shape=(
            jax.ShapeDtypeStruct((32, 1024), F32),
            jax.ShapeDtypeStruct((64, 1024), F32),
            jax.ShapeDtypeStruct((16, 512, 128), F32),
        ),
        in_specs=[half(0), half(1), tiles, any_, any_, any_, any_,
                  fixed((64, 1024)), fixed((64, 1024)), fixed((32, 1024))],
        out_specs=(
            pl.BlockSpec((32, 1024), lambda b: (0, 0)),
            pl.BlockSpec((64, 1024), lambda b: (0, 0)),
            tiles,
        ),
        scratch_shapes=[
            pltpu.VMEM((4, 128, 1024), F32),
            pltpu.VMEM((4, 128, 1024), F32),
            pltpu.VMEM((2, 8, 1024, 128), F32),
            pltpu.VMEM((1024, 1024), BF16), pltpu.VMEM((1024, 1024), BF16),
            pltpu.VMEM((1024, 1024), BF16), pltpu.VMEM((1024, 1024), BF16),
            pltpu.VMEM((ROWS, 1024), BF16), pltpu.VMEM((ROWS, 1024), BF16),
            pltpu.VMEM((ROWS, 1024), BF16), pltpu.VMEM((ROWS, 1024), BF16),
            pltpu.VMEM((512, 1024), BF16), pltpu.VMEM((512, 1024), BF16),
            pltpu.SemaphoreType.DMA((3,)),
        ],
        compiler_params=pltpu.CompilerParams(
            dimension_semantics=("arbitrary",), vmem_limit_bytes=63 * 1024 * 1024
        ),
        name="update",
    )(g, g, trailing, g, cm, cp, hh, pown, fown, iown)


def body(inverse_factor, diag_block, panel_matrix, panel_factor, trailing):
    a = lax.axis_index("prow")
    k = lax.axis_index("pcol") % 2
    first = k == 0
    p4 = panel_matrix.reshape(4, 4, 4, 1024)
    f4 = panel_factor.reshape(4, 4, 4, 1024)

    def placed(v):
        zero = jnp.zeros_like(v)
        return jnp.concatenate([jnp.where(first, v, zero), jnp.where(first, zero, v)], axis=2)

    own = placed(jnp.where(first, p4, f4))
    oth = placed(jnp.where(first, f4, p4))
    ei = lax.dynamic_slice_in_dim(inverse_factor, 128 * a, 128, 1)
    ed = lax.dynamic_slice_in_dim(diag_block, 128 * a, 128, 1)
    g, cm, cp, hh = gather(own, oth, jnp.where(first, ei, ed), jnp.where(first, ed, ei))
    red, panel, out = update(
        g, cm, cp, hh,
        panel_matrix.reshape(64, 1024), panel_factor.reshape(64, 1024), inverse_factor,
        trailing.reshape(16, 512, 128),
    )
    return red, panel.reshape(panel_matrix.shape), out.reshape(trailing.shape)


def solution(mesh):
    rows = P(None, "prow", "pcol", None)
    tiles = P(None, "prow", None, None, "pcol", None)
    return jax.shard_map(
        body,
        mesh=mesh,
        in_specs=(P("pcol", None), P("pcol", None), rows, rows, tiles),
        out_specs=(P("pcol", None), rows, tiles),
        check_vma=False,
    )
```

```python
import functools

import jax
import jax.numpy as jnp
from jax import lax
from jax.experimental import pallas as pl
from jax.experimental.pallas import tpu as pltpu
from jax.sharding import PartitionSpec as P

MESH = pl.DeviceIdType.MESH
F32 = jnp.float32
BF16 = jnp.bfloat16


def comm_kernel(own, oth, eown, eoth, g_ref, cm_ref, cp_ref, h_ref,
                merged, swap, loc_sem, pre_send, pre_recv, xh_send, xh_recv,
                z_send, z_recv, d_send, d_recv, c_send, c_recv, cd_send, cd_recv,
                e_pre, ez_send, ez_recv, ey_send, ey_recv, ed_send, ed_recv):
    a = lax.axis_index("prow")
    c = lax.axis_index("pcol")
    xl, y = a // 4, a % 4
    z, xh, k = c // 4, (c // 2) % 2, c % 2
    d = c // 2

    partner = (a, c + 1 - 2 * k)
    z_next = (a, ((z + 1) % 8) * 4 + xh * 2 + k)
    z_prev = (a, ((z + 7) % 8) * 4 + xh * 2 + k)
    x_far = (a, z * 4 + (1 - xh) * 2 + k)
    x_near = ((1 - xl) * 4 + y, c)
    y_next = (xl * 4 + (y + 1) % 4, c)
    y_prev = (xl * 4 + (y + 3) % 4, c)
    z_to = (z_next, z_prev)

    def remote(src, dst, send, recv, to):
        return pltpu.make_async_remote_copy(
            src_ref=src, dst_ref=dst, send_sem=send, recv_sem=recv, device_id=to, device_id_type=MESH
        )

    barrier = pltpu.get_barrier_semaphore()
    for to in (partner, z_next, z_prev, x_far, x_near, y_next, y_prev):
        pl.semaphore_signal(barrier, inc=1, device_id=to, device_id_type=MESH)
    pl.semaphore_wait(barrier, 7)

    def h_rows(which, block, start, size):
        return h_ref.at[which, block, pl.ds(pl.multiple_of(start, 32), size), :]

    def plane(h, t):
        return lax.rem(z + 8 - t, 8) if h == 0 else lax.rem(z + t, 8)

    def rows8(t, h, e):
        side = xh if e == 0 else 1 - xh
        return pl.ds(pl.multiple_of(16 * plane(h, t) + 8 * side, 8), 8)

    pre_e = remote(eoth, h_rows(1 - k, a, 32 * c, 32), e_pre.at[0], e_pre.at[1], partner)
    pre_e.start()
    pre = remote(oth, swap, pre_send, pre_recv, partner)
    pre.start()
    mine_e = pltpu.make_async_copy(eown, h_rows(k, a, 32 * c, 32), e_pre.at[2])
    mine_e.start()
    mine_e.wait()
    remote(eoth, h_rows(k, a, 32 * (c + 1 - 2 * k), 32), e_pre.at[0], e_pre.at[1], partner).wait_recv()
    far_e = remote(h_rows(k, a, 64 * d, 64), h_rows(k, a, 64 * d, 64), e_pre.at[3], e_pre.at[4], x_far)
    far_e.start()
    pre.wait_recv()
    merged[...] = own[...] + swap[...]

    def half(h):
        return merged.at[pl.ds(2 * h, 2)]

    def z_ref(h, t, e):
        return g_ref.at[k, pl.ds(2 * h, 2), :, rows8(t, h, e), :]

    for h in range(2):
        remote(half(h), z_ref(h, 0, 0), z_send.at[h, 0, 0], z_recv.at[h, 0, 0], z_to[h]).start()

    def far(h, e):
        return remote(half(h), z_ref(h, 0, e), xh_send.at[h], xh_recv.at[h], x_far)

    for h in range(2):
        far(h, 0).start()
    mine = [pltpu.make_async_copy(half(h), z_ref(h, 0, 0), loc_sem.at[h]) for h in range(2)]
    for h in range(2):
        mine[h].start()

    def z_copy(h, t, e):
        ref = z_ref(h, t, e)
        return remote(ref, ref, z_send.at[h, e, t], z_recv.at[h, e, t], z_to[h])

    def z_got(h, t, e):
        ref = z_ref(h, t, e)
        return remote(ref, ref, z_send.at[h, e, t - 1], z_recv.at[h, e, t - 1], z_to[h])

    def d_copy(h, t, e, which=None):
        ref = g_ref.at[k if which is None else which, pl.ds(2 * h, 2), :, rows8(t, h, e), :]
        return remote(ref, ref, d_send.at[h, t, e], d_recv.at[h, t, e], partner)

    def e_rows(which, dx, dy, h, t):
        block = lax.rem(xl + dx, 2) * 4 + lax.rem(y + dy, 4)
        return h_rows(which, block, 128 * plane(h, t), 128)

    def ez_copy(h, t):
        ref = e_rows(k, 0, 0, h, t)
        return remote(ref, ref, ez_send.at[h, t], ez_recv.at[h, t], z_to[h])

    def ez_got(h, t):
        ref = e_rows(k, 0, 0, h, t)
        return remote(ref, ref, ez_send.at[h, t - 1], ez_recv.at[h, t - 1], z_to[h])

    e_hops = (
        (0, 0, x_near, 1, 0),
        (0, 0, y_next, 0, 3),
        (0, 0, y_prev, 0, 1),
        (1, 0, y_next, 1, 3),
        (1, 0, y_prev, 1, 1),
        (0, 1, y_prev, 0, 2),
        (1, 3, y_next, 1, 2),
    )

    def e_copy(out, h, t):
        dx, dy, to, rx, ry = e_hops[out]
        ref = e_rows(k, dx, dy, h, t)
        return remote(ref, ref, ey_send.at[out, t + 4 * h], ey_recv.at[4 * rx + ry, t + 4 * h], to)

    def e_got(dx, dy, h, t):
        ref = e_rows(k, dx, dy, h, t)
        return remote(ref, ref, ey_send.at[0, t + 4 * h], ey_recv.at[4 * dx + dy, t + 4 * h], partner)

    def e_pass(dx, dy, which=None):
        block = lax.rem(xl + dx, 2) * 4 + lax.rem(y + dy, 4)
        ref = h_ref.at[k if which is None else which, block]
        return remote(ref, ref, ed_send.at[4 * dx + dy], ed_recv.at[4 * dx + dy], partner)

    def valid(h, t):
        return jnp.logical_and(t >= h, t <= 4 - h)

    def e_step(s):
        for h in range(2):
            @pl.when(s <= 4 - h)
            def _():
                ez_got(h, s).wait_recv()

                @pl.when(s < 4 - h)
                def _():
                    ez_copy(h, s).start()

                for out in range(3):
                    e_copy(out, h, s).start()

            @pl.when(valid(h, s - 1))
            def _():
                t = jnp.maximum(s - 1, h)
                e_got(1, 0, h, t).wait_recv()
                e_copy(3, h, t).start()
                e_copy(4, h, t).start()
                e_got(0, 1, h, t).wait_recv()
                e_copy(5, h, t).start()
                e_got(0, 3, h, t).wait_recv()

            @pl.when(valid(h, s - 2))
            def _():
                t = jnp.maximum(s - 2, h)
                e_got(1, 3, h, t).wait_recv()
                e_copy(6, h, t).start()
                e_got(1, 1, h, t).wait_recv()

            @pl.when(valid(h, s - 3))
            def _():
                t = jnp.maximum(s - 3, h)
                e_got(0, 2, h, t).wait_recv()
                e_got(1, 2, h, t).wait_recv()

        @pl.when(s == 4)
        def _():
            e_pass(0, 0).start()

        @pl.when(s == 5)
        def _():
            for dx, dy in ((1, 0), (0, 1), (0, 3)):
                e_pass(dx, dy).start()

        @pl.when(s == 6)
        def _():
            for dx, dy in ((1, 3), (1, 1)):
                e_pass(dx, dy).start()

        @pl.when(s == 7)
        def _():
            for dx, dy in ((0, 2), (1, 2)):
                e_pass(dx, dy).start()

    q = z // 2
    in_plane = xl == z % 2
    y_out = (2, 1)

    def place(m):
        return lax.rem(y - (2 * xh + m) + 4, 4)

    def c_copy(m, h, t, e, out, from_g=False):
        dst = cm_ref.at[m, pl.ds(2 * h, 2), rows8(t, h, e), :]
        src = g_ref.at[k, pl.ds(2 * h, 2), q, rows8(t, h, e), :] if from_g else dst
        to = (x_near, y_next, y_prev)[out]
        return remote(src, dst, c_send.at[m, h, t, e, out], c_recv.at[m, h, t, e], to)

    def cd_copy(m, h, t, e):
        src = cm_ref.at[m, pl.ds(2 * h, 2), rows8(t, h, e), :]
        dst = cp_ref.at[pl.ds(2 * h, 2), rows8(t, h, e), :]
        return remote(src, dst, cd_send.at[h, t, e], cd_recv.at[h, t, e], partner)

    def is_source(m):
        return jnp.logical_and(in_plane, place(m) == 0)

    def off_root(m):
        return jnp.logical_and(jnp.logical_not(in_plane), place(m) == 0)

    def relays(m):
        return place(m) == (3, 1)[m]

    def source_sends(t, e):
        for m in range(2):
            @pl.when(is_source(m))
            def _():
                for h in range(2):
                    for out in range(3):
                        c_copy(m, h, t, e, out, True).start()

    def take_columns(t, e, lag):
        for m in range(2):
            r = place(m)
            when = (
                jnp.logical_or(off_root(m), jnp.logical_and(in_plane, r % 2 == 1)),
                jnp.logical_or(
                    jnp.logical_and(in_plane, r == 2),
                    jnp.logical_and(jnp.logical_not(in_plane), r % 2 == 1),
                ),
                jnp.logical_and(jnp.logical_not(in_plane), r == 2),
            )[lag - 1]

            @pl.when(jnp.logical_and(when, t >= 0))
            def _():
                s = jnp.maximum(t, 0)
                for h in range(2):
                    c_copy(m, h, s, e, 0).wait_recv()

                    @pl.when(r == 0)
                    def _():
                        for out in (1, 2):
                            c_copy(m, h, s, e, out).start()

                    @pl.when(relays(m))
                    def _():
                        c_copy(m, h, s, e, y_out[m]).start()

                    @pl.when(k != m)
                    def _():
                        cd_copy(m, h, s, e).start()

    def after(t, e):
        for h in range(2):
            d_copy(h, t, e).start()
        source_sends(t, e)

    mine[0].wait()
    mine[1].wait()
    df = d + 1 - 2 * xh
    remote(
        h_rows(k, a, 64 * df, 64), h_rows(k, a, 64 * df, 64), e_pre.at[3], e_pre.at[4], x_far
    ).wait_recv()
    for h in range(2):
        ez_copy(h, 0).start()
    for out in range(3):
        e_copy(out, 0, 0).start()
    after(0, 0)

    def step(s, carry):
        for h in range(2):
            z_got(h, s, 0).wait_recv()

            @pl.when(s < 7)
            def _():
                z_copy(h, s, 0).start()

        after(s, 0)
        for lag in (1, 2, 3):
            take_columns(s - lag, 0, lag)
        e_step(s)
        t = s - 1
        for h in range(2):
            @pl.when(t == 0)
            def _():
                far(h, 1).wait_recv()

            @pl.when(t > 0)
            def _():
                z_got(h, jnp.maximum(t, 1), 1).wait_recv()

            z_copy(h, t, 1).start()

        after(t, 1)
        for lag in (1, 2, 3):
            take_columns(t - lag, 1, lag)
        return carry

    lax.fori_loop(1, 8, step, 0)
    last = jnp.int32(7)
    for h in range(2):
        z_got(h, last, 1).wait_recv()
    after(last, 1)
    for lag in (1, 2, 3):
        for back in range(lag, -1, -1):
            if back < lag:
                take_columns(last - back, 0, lag)
            take_columns(last - back, 1, lag)

    pre_e.wait_send()
    pre.wait_send()
    far_e.wait_send()
    for h in range(2):
        far(h, 0).wait_send()
        for t in range(4 - h):
            ez_copy(h, t).wait_send()
        for t in range(h, 5 - h):
            for out in range(7):
                e_copy(out, h, t).wait_send()
    for dx in range(2):
        for dy in range(4):
            e_pass(dx, dy).wait_send()
            e_pass(dx, dy, 1 - k).wait_recv()

    def finish(t, carry):
        for e in range(2):
            for h in range(2):
                @pl.when(t < 7)
                def _():
                    z_copy(h, t, e).wait_send()

                d_copy(h, t, e).wait_send()
                d_copy(h, t, e, 1 - k).wait_recv()
                for m in range(2):
                    @pl.when(is_source(m))
                    def _():
                        for out in range(3):
                            c_copy(m, h, t, e, out, True).wait_send()

                    @pl.when(off_root(m))
                    def _():
                        for out in (1, 2):
                            c_copy(m, h, t, e, out).wait_send()

                    @pl.when(relays(m))
                    def _():
                        c_copy(m, h, t, e, y_out[m]).wait_send()

                    @pl.when(jnp.logical_not(is_source(m)))
                    def _():
                        @pl.when(k != m)
                        def _():
                            cd_copy(m, h, t, e).wait_send()

                        @pl.when(k == m)
                        def _():
                            cd_copy(m, h, t, e).wait_recv()

        return carry

    lax.fori_loop(0, 8, finish, 0)


def gather(own, oth, eown, eoth):
    dma = pltpu.SemaphoreType.DMA
    return pl.pallas_call(
        comm_kernel,
        out_shape=(
            jax.ShapeDtypeStruct((2, 4, 4, 128, 1024), F32),
            jax.ShapeDtypeStruct((2, 4, 128, 1024), F32),
            jax.ShapeDtypeStruct((4, 128, 1024), F32),
            jax.ShapeDtypeStruct((2, 8, 1024, 128), F32),
        ),
        in_specs=[pl.BlockSpec(memory_space=pltpu.VMEM)] * 4,
        out_specs=(pl.BlockSpec(memory_space=pl.ANY),) * 4,
        scratch_shapes=[
            pltpu.VMEM((4, 4, 8, 1024), F32),
            pltpu.VMEM((4, 4, 8, 1024), F32),
            dma((2,)), dma, dma, dma((2,)), dma((2,)),
            dma((2, 2, 7)), dma((2, 2, 7)),
            dma((2, 8, 2)), dma((2, 8, 2)),
            dma((2, 2, 8, 2, 3)), dma((2, 2, 8, 2)),
            dma((2, 8, 2)), dma((2, 8, 2)),
            dma((5,)),
            dma((2, 4)), dma((2, 4)),
            dma((7, 8)), dma((8, 8)),
            dma((8,)), dma((8,)),
        ],
        compiler_params=pltpu.CompilerParams(collective_id=0, has_side_effects=True),
        name="gather",
    )(own, oth, eown, eoth)


def split(v):
    hi = v.astype(BF16)
    return hi, (v - hi.astype(F32)).astype(BF16)


def dot3(x, y, contract):
    (xh, xlo), (yh, ylo) = x, y
    dims = (((1,), (contract,)), ((), ()))
    dot = functools.partial(lax.dot_general, dimension_numbers=dims, preferred_element_type=F32)
    return dot(xh, yh) + dot(xlo, yh) + dot(xh, ylo)


ROWS = 608


def update_kernel(pb, fb, tr, g_ref, cm_ref, cp_ref, h_ref, pown, fown, iown,
                  red_ref, panel_ref, out_ref,
                  pc, fc, hv, ih, il, dh, dl, uh, ul, th, tl, vh, vl, sems):
    b = pl.program_id(0)
    a = lax.axis_index("prow")
    c = lax.axis_index("pcol")
    z, xh, k = c // 4, (c // 2) % 2, c % 2
    source = a == (z % 2) * 4 + 2 * xh + k

    @pl.when(b == 0)
    def _():
        load_h = pltpu.make_async_copy(h_ref, hv, sems.at[2])
        load_h.start()

        @pl.when(source)
        def _():
            pltpu.make_async_copy(g_ref.at[0, :, z // 2], pc, sems.at[0]).start()
            pltpu.make_async_copy(g_ref.at[1, :, z // 2], fc, sems.at[1]).start()

        @pl.when(jnp.logical_not(source))
        def _():
            @pl.when(k == 0)
            def _():
                pltpu.make_async_copy(cm_ref.at[0], pc, sems.at[0]).start()
                pltpu.make_async_copy(cp_ref, fc, sems.at[1]).start()

            @pl.when(k == 1)
            def _():
                pltpu.make_async_copy(cp_ref, pc, sems.at[0]).start()
                pltpu.make_async_copy(cm_ref.at[1], fc, sems.at[1]).start()

        load_h.wait()
        for g in range(8):
            lanes = slice(128 * g, 128 * g + 128)
            hi, lo = split(hv[0, g])
            ih[:, lanes] = hi
            il[:, lanes] = lo
            hi, lo = split(hv[1, g])
            dh[:, lanes] = hi
            dl[:, lanes] = lo
        pltpu.make_async_copy(cm_ref.at[0], pc, sems.at[0]).wait()
        pltpu.make_async_copy(cm_ref.at[0], fc, sems.at[1]).wait()

        hi, lo = split(fc[...].reshape(512, 1024))
        th[0:512] = hi
        tl[0:512] = lo
        hi, lo = split(fown[...])
        th[512:576] = hi
        tl[512:576] = lo
        for n in range(4):
            cols = slice(256 * n, 256 * n + 256)
            deep = slice(256 * n, 1024)
            u = dot3(
                (th[0:576, deep], tl[0:576, deep]), (ih[deep, cols], il[deep, cols]), 0
            )
            hi, lo = split(u)
            uh[0:576, cols] = hi
            ul[0:576, cols] = lo
        hi, lo = split(iown[...])
        uh[576:608] = hi
        ul[576:608] = lo
        for n in range(4):
            cols = slice(256 * n, 256 * n + 256)
            start = jnp.concatenate(
                [pc[:, :, cols].reshape(512, 256), pown[:, cols], jnp.zeros((32, 256), F32)]
            )
            t = start - dot3((uh[...], ul[...]), (dh[:, cols], dl[:, cols]), 0)
            hi, lo = split(t)
            th[:, cols] = hi
            tl[:, cols] = lo
        for n in range(4):
            cols = slice(256 * n, 256 * n + 256)
            deep = slice(0, 256 * n + 256)
            v = dot3((th[:, deep], tl[:, deep]), (ih[cols, deep], il[cols, deep]), 1)
            hi, lo = split(v[0:512])
            vh[:, cols] = hi
            vl[:, cols] = lo
            panel_ref[:, cols] = v[512:576]
            red_ref[:, cols] = -v[576:608]

    for n in range(4):
        @pl.when(b == n)
        def _():
            wide = slice(0, 128 * n + 128)
            for q in range(2):
                first = split(pb[0, 0, 2 * q:2 * q + 2].reshape(256, 1024))
                second = split(fb[0, 0, 2 * q:2 * q + 2].reshape(256, 1024))
                total = dot3(first, (uh[wide], ul[wide]), 1) + dot3(second, (vh[wide], vl[wide]), 1)
                for p in range(2):
                    i = 2 * q + p
                    lower = 8 * i + a >= c
                    for j in range(4):
                        at = pl.ds(j, 128, stride=4)
                        held = tr[i, at, :]
                        if j <= n:
                            new = held - total[128 * p:128 * p + 128, 128 * j:128 * j + 128]
                            held = jnp.where(lower, new, held) if j == n else new
                        out_ref[i, at, :] = held


def update(g, cm, cp, hh, pown, fown, iown, trailing):
    any_ = pl.BlockSpec(memory_space=pl.ANY)
    fixed = lambda shape: pl.BlockSpec(shape, lambda b: (0,) * len(shape), pipeline_mode=pl.Buffered(1))
    half = lambda which: pl.BlockSpec((1, 1, 4, 128, 1024), lambda b: (which, b, 0, 0, 0))
    tiles = pl.BlockSpec((4, 512, 128), lambda b: (b, 0, 0))
    return pl.pallas_call(
        update_kernel,
        grid=(4,),
        out_shape=(
            jax.ShapeDtypeStruct((32, 1024), F32),
            jax.ShapeDtypeStruct((64, 1024), F32),
            jax.ShapeDtypeStruct((16, 512, 128), F32),
        ),
        in_specs=[half(0), half(1), tiles, any_, any_, any_, any_,
                  fixed((64, 1024)), fixed((64, 1024)), fixed((32, 1024))],
        out_specs=(
            pl.BlockSpec((32, 1024), lambda b: (0, 0)),
            pl.BlockSpec((64, 1024), lambda b: (0, 0)),
            tiles,
        ),
        scratch_shapes=[
            pltpu.VMEM((4, 128, 1024), F32),
            pltpu.VMEM((4, 128, 1024), F32),
            pltpu.VMEM((2, 8, 1024, 128), F32),
            pltpu.VMEM((1024, 1024), BF16), pltpu.VMEM((1024, 1024), BF16),
            pltpu.VMEM((1024, 1024), BF16), pltpu.VMEM((1024, 1024), BF16),
            pltpu.VMEM((ROWS, 1024), BF16), pltpu.VMEM((ROWS, 1024), BF16),
            pltpu.VMEM((ROWS, 1024), BF16), pltpu.VMEM((ROWS, 1024), BF16),
            pltpu.VMEM((512, 1024), BF16), pltpu.VMEM((512, 1024), BF16),
            pltpu.SemaphoreType.DMA((3,)),
        ],
        compiler_params=pltpu.CompilerParams(
            dimension_semantics=("arbitrary",), vmem_limit_bytes=63 * 1024 * 1024
        ),
        name="update",
    )(g, g, trailing, g, cm, cp, hh, pown, fown, iown)


def body(inverse_factor, diag_block, panel_matrix, panel_factor, trailing):
    a = lax.axis_index("prow")
    k = lax.axis_index("pcol") % 2
    first = k == 0
    p4 = panel_matrix.reshape(4, 4, 4, 1024)
    f4 = panel_factor.reshape(4, 4, 4, 1024)

    def placed(v):
        zero = jnp.zeros_like(v)
        return jnp.concatenate([jnp.where(first, v, zero), jnp.where(first, zero, v)], axis=2)

    own = placed(jnp.where(first, p4, f4))
    oth = placed(jnp.where(first, f4, p4))
    ei = lax.dynamic_slice_in_dim(inverse_factor, 128 * a, 128, 1)
    ed = lax.dynamic_slice_in_dim(diag_block, 128 * a, 128, 1)
    g, cm, cp, hh = gather(own, oth, jnp.where(first, ei, ed), jnp.where(first, ed, ei))
    red, panel, out = update(
        g, cm, cp, hh,
        panel_matrix.reshape(64, 1024), panel_factor.reshape(64, 1024), inverse_factor,
        trailing.reshape(16, 512, 128),
    )
    return red, panel.reshape(panel_matrix.shape), out.reshape(trailing.shape)


def solution(mesh):
    rows = P(None, "prow", "pcol", None)
    tiles = P(None, "prow", None, None, "pcol", None)
    return jax.shard_map(
        body,
        mesh=mesh,
        in_specs=(P("pcol", None), P("pcol", None), rows, rows, tiles),
        out_specs=(P("pcol", None), rows, tiles),
        check_vma=False,
    )
```

```python
import functools

import jax
import jax.numpy as jnp
from jax import lax
from jax.experimental import pallas as pl
from jax.experimental.pallas import tpu as pltpu
from jax.sharding import PartitionSpec as P

MESH = pl.DeviceIdType.MESH
F32 = jnp.float32
BF16 = jnp.bfloat16


E_PASSES = (
    (4, ((0, 0),)),
    (5, ((1, 0), (0, 1), (0, 3))),
    (6, ((1, 3), (1, 1))),
    (7, ((0, 2), (1, 2))),
)


def comm_kernel(p_ref, f_ref, inv_ref, diag_ref, g_ref, cm_ref, cp_ref, h_ref,
                merged, swap, loc_sem, pre_send, pre_recv, xh_send, xh_recv,
                z_send, z_recv, d_send, d_recv, c_send, c_recv, cf_send, cd_send, cd_recv,
                xf_send, xf_recv, e_pre, ez_send, ez_recv, ey_send, ey_recv, ed_send, ed_recv):
    a = lax.axis_index("prow")
    c = lax.axis_index("pcol")
    xl, y = a // 4, a % 4
    z, xh, k = c // 4, (c // 2) % 2, c % 2
    d = c // 2

    partner = (a, c + 1 - 2 * k)
    z_next = (a, ((z + 1) % 8) * 4 + xh * 2 + k)
    z_prev = (a, ((z + 7) % 8) * 4 + xh * 2 + k)
    x_far = (a, z * 4 + (1 - xh) * 2 + k)
    x_near = ((1 - xl) * 4 + y, c)
    x_side = ((1 - xl) * 4 + y, z * 4 + (1 - xh) * 2 + k)
    y_next = (xl * 4 + (y + 1) % 4, c)
    y_prev = (xl * 4 + (y + 3) % 4, c)
    z_to = (z_next, z_prev)

    def remote(src, dst, send, recv, to):
        return pltpu.make_async_remote_copy(
            src_ref=src, dst_ref=dst, send_sem=send, recv_sem=recv, device_id=to, device_id_type=MESH
        )

    barrier = pltpu.get_barrier_semaphore()
    for to in (partner, z_next, z_prev, x_far, x_near, x_side, y_next, y_prev):
        pl.semaphore_signal(barrier, inc=1, device_id=to, device_id_type=MESH)
    pl.semaphore_wait(barrier, 8)

    def h_rows(which, block, start, size):
        return h_ref.at[which, block, pl.ds(pl.multiple_of(start, 32), size), :]

    def plane(h, t):
        return lax.rem(z + 8 - t, 8) if h == 0 else lax.rem(z + t, 8)

    def rows8(t, h, e):
        side = lax.rem(xh + e, 2)
        return pl.ds(pl.multiple_of(16 * plane(h, t) + 8 * side, 8), 8)

    lanes = pl.ds(pl.multiple_of(128 * a, 128), 128)
    pairs = ((p_ref, f_ref, inv_ref, diag_ref), (f_ref, p_ref, diag_ref, inv_ref))
    for me in range(2):
        @pl.when(k == me)
        def _():
            _, other, e_own, e_other = pairs[me]
            remote(
                e_other.at[:, lanes], h_rows(1 - me, a, 32 * c, 32), e_pre.at[0], e_pre.at[1], partner
            ).start()
            remote(other, swap, pre_send, pre_recv, partner).start()
            pltpu.make_async_copy(e_own.at[:, lanes], h_rows(me, a, 32 * c, 32), e_pre.at[2]).start()

    pre = remote(f_ref, swap, pre_send, pre_recv, partner)
    mine_e = pltpu.make_async_copy(inv_ref.at[:, lanes], h_rows(k, a, 32 * c, 32), e_pre.at[2])
    mine_e.wait()
    pre_e = remote(
        inv_ref.at[:, lanes], h_rows(k, a, 32 * (c + 1 - 2 * k), 32), e_pre.at[0], e_pre.at[1], partner
    )
    pre_e.wait_recv()
    far_e = remote(h_rows(k, a, 64 * d, 64), h_rows(k, a, 64 * d, 64), e_pre.at[3], e_pre.at[4], x_far)
    far_e.start()
    pre.wait_recv()
    merged[:, :, 0:4, :] = jnp.where(k == 0, p_ref[...], swap[...])
    merged[:, :, 4:8, :] = jnp.where(k == 0, swap[...], f_ref[...])

    def half(h):
        return merged.at[pl.ds(2 * h, 2)]

    def z_ref(h, t, e):
        return g_ref.at[k, pl.ds(2 * h, 2), pl.ds(0, 4 - e), rows8(t, h, e), :]

    for h in range(2):
        remote(half(h), z_ref(h, 0, 0), z_send.at[h, 0, 0], z_recv.at[h, 0, 0], z_to[h]).start()

    def far(h, e):
        ref = g_ref.at[k, pl.ds(2 * h, 2), :, rows8(0, h, e), :]
        return remote(half(h), ref, xh_send.at[h], xh_recv.at[h], x_far)

    def xf_copy(h, t, e):
        ref = g_ref.at[k, pl.ds(2 * h, 2), pl.ds(3, 1), rows8(t, h, e), :]
        return remote(ref, ref, xf_send.at[h, t], xf_recv.at[h, t], x_far)

    for h in range(2):
        far(h, 0).start()
    mine = [pltpu.make_async_copy(half(h), z_ref(h, 0, 0), loc_sem.at[h]) for h in range(2)]
    for h in range(2):
        mine[h].start()

    def z_copy(h, t, e):
        ref = z_ref(h, t, e)
        return remote(ref, ref, z_send.at[h, e, t], z_recv.at[h, e, t], z_to[h])

    def z_got(h, t, e):
        ref = z_ref(h, t, e)
        return remote(ref, ref, z_send.at[h, e, t - 1], z_recv.at[h, e, t - 1], z_to[h])

    def d_copy(h, t, e, which=None):
        ref = g_ref.at[k if which is None else which, pl.ds(2 * h, 2), :, rows8(t, h, e), :]
        return remote(ref, ref, d_send.at[h, t, e], d_recv.at[h, t, e], partner)

    def e_rows(which, dx, dy, h, t):
        block = lax.rem(xl + dx, 2) * 4 + lax.rem(y + dy, 4)
        return h_rows(which, block, 128 * plane(h, t), 128)

    def ez_copy(h, t):
        ref = e_rows(k, 0, 0, h, t)
        return remote(ref, ref, ez_send.at[h, t], ez_recv.at[h, t], z_to[h])

    def ez_got(h, t):
        ref = e_rows(k, 0, 0, h, t)
        return remote(ref, ref, ez_send.at[h, t - 1], ez_recv.at[h, t - 1], z_to[h])

    e_hops = (
        (0, 0, x_near, 1, 0),
        (0, 0, y_next, 0, 3),
        (0, 0, y_prev, 0, 1),
        (1, 0, y_next, 1, 3),
        (1, 0, y_prev, 1, 1),
        (0, 1, y_prev, 0, 2),
        (1, 3, y_next, 1, 2),
    )

    def e_copy(out, h, t):
        dx, dy, to, rx, ry = e_hops[out]
        ref = e_rows(k, dx, dy, h, t)
        return remote(ref, ref, ey_send.at[out, t + 4 * h], ey_recv.at[4 * rx + ry, t + 4 * h], to)

    def e_got(dx, dy, h, t):
        ref = e_rows(k, dx, dy, h, t)
        return remote(ref, ref, ey_send.at[0, t + 4 * h], ey_recv.at[4 * dx + dy, t + 4 * h], partner)

    def blk(dx, dy):
        return lax.rem(xl + dx, 2) * 4 + lax.rem(y + dy, 4)

    def lower(dx, dy, h, t):
        return plane(h, t) >= blk(dx, dy)

    def valid(h, t):
        return jnp.logical_and(t >= h, t <= 4 - h)

    def e_take(out_got, outs, h, t):
        dx, dy = out_got

        @pl.when(lower(dx, dy, h, t))
        def _():
            e_got(dx, dy, h, t).wait_recv()
            for out in outs:
                e_copy(out, h, t).start()

    def e_step(s):
        for h in range(2):
            @pl.when(jnp.logical_and(s <= 4 - h, lower(0, 0, h, s)))
            def _():
                ez_got(h, s).wait_recv()

                @pl.when(s < 4 - h)
                def _():
                    ez_copy(h, s).start()

                for out in range(3):
                    e_copy(out, h, s).start()

            @pl.when(valid(h, s - 1))
            def _():
                t = jnp.maximum(s - 1, h)
                e_take((1, 0), (3, 4), h, t)
                e_take((0, 1), (5,), h, t)
                e_take((0, 3), (), h, t)

            @pl.when(valid(h, s - 2))
            def _():
                t = jnp.maximum(s - 2, h)
                e_take((1, 3), (6,), h, t)
                e_take((1, 1), (), h, t)

            @pl.when(valid(h, s - 3))
            def _():
                t = jnp.maximum(s - 3, h)
                e_take((0, 2), (), h, t)
                e_take((1, 2), (), h, t)

        for at, blocks in E_PASSES:
            @pl.when(s == at)
            def _():
                e_pass_all(blocks, lambda copy: copy.start())

    def e_piece(dx, dy, p, which):
        ref = h_rows(which, blk(dx, dy), 128 * p, 128)
        return remote(ref, ref, ed_send.at[4 * dx + dy, p], ed_recv.at[4 * dx + dy, p], partner)

    def e_pass_all(blocks, act, which=None):
        def piece(p, carry):
            for dx, dy in blocks:
                @pl.when(p >= blk(dx, dy))
                def _():
                    act(e_piece(dx, dy, p, k if which is None else which))

            return carry

        lax.fori_loop(0, 8, piece, 0)

    q = z // 2
    in_plane = xl == z % 2
    y_out = (2, 1)

    def place(m):
        return lax.rem(y - (2 * xh + m) + 4, 4)

    def c_copy(m, h, t, e, out, from_g=False):
        dst = cm_ref.at[m, pl.ds(2 * h, 2), rows8(t, h, e), :]
        src = g_ref.at[k, pl.ds(2 * h, 2), q, rows8(t, h, e), :] if from_g else dst
        to = (x_near, y_next, y_prev)[out]
        return remote(src, dst, c_send.at[m, h, t, e, out], c_recv.at[m, h, t, e], to)

    def cd_copy(m, h, t, e):
        src = cm_ref.at[m, pl.ds(2 * h, 2), rows8(t, h, e), :]
        dst = cp_ref.at[pl.ds(2 * h, 2), rows8(t, h, e), :]
        return remote(src, dst, cd_send.at[h, t, e], cd_recv.at[h, t, e], partner)

    def is_source(m):
        return jnp.logical_and(in_plane, place(m) == 0)

    def off_root(m):
        return jnp.logical_and(jnp.logical_not(in_plane), place(m) == 0)

    def relays(m):
        return place(m) == (3, 1)[m]

    def is_side(m):
        return jnp.logical_and(in_plane, y == 2 * (1 - xh) + m)

    def side_copy(m, t, e):
        src = g_ref.at[k, pl.ds(2, 2), q, rows8(t, 1, e), :]
        dst = cm_ref.at[m, pl.ds(2, 2), rows8(t, 1, e), :]
        return remote(src, dst, cf_send.at[m, t, e], c_recv.at[m, 1, t, 1 - e], x_side)

    def source_sends(t, e):
        for m in range(2):
            @pl.when(is_source(m))
            def _():
                for h in range(2):
                    for out in range(h, 3):
                        c_copy(m, h, t, e, out, True).start()

            @pl.when(is_side(m))
            def _():
                side_copy(m, t, e).start()

    def take_columns(t, slot, lag):
        for m in range(2):
            r = place(m)
            when = (
                jnp.logical_or(off_root(m), jnp.logical_and(in_plane, r % 2 == 1)),
                jnp.logical_or(
                    jnp.logical_and(in_plane, r == 2),
                    jnp.logical_and(jnp.logical_not(in_plane), r % 2 == 1),
                ),
                jnp.logical_and(jnp.logical_not(in_plane), r == 2),
            )[lag - 1]

            @pl.when(jnp.logical_and(when, t >= 0))
            def _():
                s = jnp.maximum(t, 0)
                for h in range(2):
                    e = jnp.where(in_plane, slot, 1 - slot) if h == 1 else slot
                    c_copy(m, h, s, e, 0).wait_recv()

                    @pl.when(r == 0)
                    def _():
                        for out in (1, 2):
                            c_copy(m, h, s, e, out).start()

                    @pl.when(relays(m))
                    def _():
                        c_copy(m, h, s, e, y_out[m]).start()

                    @pl.when(k != m)
                    def _():
                        cd_copy(m, h, s, e).start()

    def after(t, e):
        for h in range(2):
            d_copy(h, t, e).start()
        source_sends(t, e)

    mine[0].wait()
    mine[1].wait()
    df = d + 1 - 2 * xh
    remote(
        h_rows(k, a, 64 * df, 64), h_rows(k, a, 64 * df, 64), e_pre.at[3], e_pre.at[4], x_far
    ).wait_recv()
    @pl.when(lower(0, 0, 0, 0))
    def _():
        for h in range(2):
            ez_copy(h, 0).start()
        for out in range(3):
            e_copy(out, 0, 0).start()

    after(0, 0)

    def step(s, carry):
        for h in range(2):
            z_got(h, s, 0).wait_recv()

            @pl.when(s < 7)
            def _():
                z_copy(h, s, 0).start()

            xf_copy(h, s, 0).start()

        after(s, 0)
        for lag in (1, 2, 3):
            take_columns(s - lag, 0, lag)
        e_step(s)
        t = s - 1
        for h in range(2):
            @pl.when(t == 0)
            def _():
                far(h, 1).wait_recv()

            @pl.when(t > 0)
            def _():
                z_got(h, jnp.maximum(t, 1), 1).wait_recv()

            z_copy(h, t, 1).start()

        for h in range(2):
            @pl.when(t > 0)
            def _():
                xf_copy(h, t, 1).wait_recv()

        after(t, 1)
        for lag in (1, 2, 3):
            take_columns(t - lag, 1, lag)
        return carry

    lax.fori_loop(1, 8, step, 0)
    last = jnp.int32(7)
    for h in range(2):
        z_got(h, last, 1).wait_recv()
        xf_copy(h, last, 1).wait_recv()
    after(last, 1)
    for lag in (1, 2, 3):
        for back in range(lag, -1, -1):
            if back < lag:
                take_columns(last - back, 0, lag)
            take_columns(last - back, 1, lag)

    pre_e.wait_send()
    pre.wait_send()
    far_e.wait_send()
    for h in range(2):
        far(h, 0).wait_send()
        for t in range(5 - h):
            if t < 4 - h:
                @pl.when(lower(0, 0, h, t))
                def _():
                    ez_copy(h, t).wait_send()

            if t >= h:
                for out in range(7):
                    @pl.when(lower(*e_hops[out][:2], h, t))
                    def _():
                        e_copy(out, h, t).wait_send()

    for _, blocks in E_PASSES:
        e_pass_all(blocks, lambda copy: copy.wait_send())
        e_pass_all(blocks, lambda copy: copy.wait_recv(), 1 - k)

    def finish(t, carry):
        for e in range(2):
            for h in range(2):
                @pl.when(t < 7)
                def _():
                    z_copy(h, t, e).wait_send()

                if e == 0:
                    @pl.when(t > 0)
                    def _():
                        xf_copy(h, t, 0).wait_send()

                d_copy(h, t, e).wait_send()
                d_copy(h, t, e, 1 - k).wait_recv()
                for m in range(2):
                    if h == 1:
                        @pl.when(is_side(m))
                        def _():
                            side_copy(m, t, e).wait_send()

                    @pl.when(is_source(m))
                    def _():
                        for out in range(h, 3):
                            c_copy(m, h, t, e, out, True).wait_send()

                    @pl.when(off_root(m))
                    def _():
                        for out in (1, 2):
                            c_copy(m, h, t, e, out).wait_send()

                    @pl.when(relays(m))
                    def _():
                        c_copy(m, h, t, e, y_out[m]).wait_send()

                    @pl.when(jnp.logical_not(is_source(m)))
                    def _():
                        @pl.when(k != m)
                        def _():
                            cd_copy(m, h, t, e).wait_send()

                        @pl.when(k == m)
                        def _():
                            cd_copy(m, h, t, e).wait_recv()

        return carry

    lax.fori_loop(0, 8, finish, 0)


def gather(p4, f4, inverse_factor, diag_block):
    dma = pltpu.SemaphoreType.DMA
    return pl.pallas_call(
        comm_kernel,
        out_shape=(
            jax.ShapeDtypeStruct((2, 4, 4, 128, 1024), F32),
            jax.ShapeDtypeStruct((2, 4, 128, 1024), F32),
            jax.ShapeDtypeStruct((4, 128, 1024), F32),
            jax.ShapeDtypeStruct((2, 8, 1024, 128), F32),
        ),
        in_specs=[pl.BlockSpec(memory_space=pltpu.VMEM)] * 4,
        out_specs=(pl.BlockSpec(memory_space=pl.ANY),) * 4,
        scratch_shapes=[
            pltpu.VMEM((4, 4, 8, 1024), F32),
            pltpu.VMEM((4, 4, 4, 1024), F32),
            dma((2,)), dma, dma, dma((2,)), dma((2,)),
            dma((2, 2, 7)), dma((2, 2, 7)),
            dma((2, 8, 2)), dma((2, 8, 2)),
            dma((2, 2, 8, 2, 3)), dma((2, 2, 8, 2)), dma((2, 8, 2)),
            dma((2, 8, 2)), dma((2, 8, 2)),
            dma((2, 8)), dma((2, 8)),
            dma((5,)),
            dma((2, 4)), dma((2, 4)),
            dma((7, 8)), dma((8, 8)),
            dma((8, 8)), dma((8, 8)),
        ],
        compiler_params=pltpu.CompilerParams(collective_id=0, has_side_effects=True),
        name="gather",
    )(p4, f4, inverse_factor, diag_block)


def split(v):
    hi = v.astype(BF16)
    return hi, (v - hi.astype(F32)).astype(BF16)


def dot3(x, y, contract):
    (xh, xlo), (yh, ylo) = x, y
    dims = (((1,), (contract,)), ((), ()))
    dot = functools.partial(lax.dot_general, dimension_numbers=dims, preferred_element_type=F32)
    return dot(xh, yh) + dot(xlo, yh) + dot(xh, ylo)


ROWS = 608


def update_kernel(pb, fb, tr, g_ref, cm_ref, cp_ref, h_ref, pown, fown, iown,
                  red_ref, panel_ref, out_ref,
                  pc, fc, po, hv, ih, il, dh, dl, uh, ul, th, tl, vh, vl, sems):
    b = pl.program_id(0)
    a = lax.axis_index("prow")
    c = lax.axis_index("pcol")
    z, xh, k = c // 4, (c // 2) % 2, c % 2
    source = a == (z % 2) * 4 + 2 * xh + k

    @pl.when(b == 0)
    def _():
        load_h = pltpu.make_async_copy(h_ref, hv, sems.at[2])
        load_h.start()

        @pl.when(source)
        def _():
            pltpu.make_async_copy(g_ref.at[0, :, z // 2], pc, sems.at[0]).start()
            pltpu.make_async_copy(g_ref.at[1, :, z // 2], fc, sems.at[1]).start()

        @pl.when(jnp.logical_not(source))
        def _():
            @pl.when(k == 0)
            def _():
                pltpu.make_async_copy(cm_ref.at[0], pc, sems.at[0]).start()
                pltpu.make_async_copy(cp_ref, fc, sems.at[1]).start()

            @pl.when(k == 1)
            def _():
                pltpu.make_async_copy(cp_ref, pc, sems.at[0]).start()
                pltpu.make_async_copy(cm_ref.at[1], fc, sems.at[1]).start()

        load_h.wait()
        for g in range(8):
            lanes = slice(128 * g, 128 * g + 128)
            deep = slice(128 * g, 1024)
            hi, lo = split(hv[0, g, deep])
            ih[deep, lanes] = hi
            il[deep, lanes] = lo
            hi, lo = split(hv[1, g, deep])
            dh[deep, lanes] = hi
            dl[deep, lanes] = lo
            if g % 2 == 1:
                top = slice(128 * g - 128, 128 * g)
                ih[top, lanes] = jnp.zeros((128, 128), BF16)
                il[top, lanes] = jnp.zeros((128, 128), BF16)
            for r in range(g + 1, 8):
                rows = slice(128 * r, 128 * r + 128)
                hi, lo = split(hv[1, g, rows].T)
                dh[lanes, rows] = hi
                dl[lanes, rows] = lo
        pltpu.make_async_copy(cm_ref.at[0], pc, sems.at[0]).wait()
        pltpu.make_async_copy(cm_ref.at[0], fc, sems.at[1]).wait()

        hi, lo = split(fc[...].reshape(512, 1024))
        th[0:512] = hi
        tl[0:512] = lo
        for i in range(16):
            po[4 * i:4 * i + 4] = fown[i]
        hi, lo = split(po[...])
        th[512:576] = hi
        tl[512:576] = lo
        for i in range(16):
            po[4 * i:4 * i + 4] = pown[i]
        for n in range(4):
            cols = slice(256 * n, 256 * n + 256)
            deep = slice(256 * n, 1024)
            u = dot3(
                (th[0:576, deep], tl[0:576, deep]), (ih[deep, cols], il[deep, cols]), 0
            )
            hi, lo = split(u)
            uh[0:576, cols] = hi
            ul[0:576, cols] = lo
        hi, lo = split(iown[...])
        uh[576:608] = hi
        ul[576:608] = lo
        for n in range(4):
            cols = slice(256 * n, 256 * n + 256)
            start = jnp.concatenate(
                [pc[:, :, cols].reshape(512, 256), po[:, cols], jnp.zeros((32, 256), F32)]
            )
            t = start - dot3((uh[...], ul[...]), (dh[:, cols], dl[:, cols]), 0)
            hi, lo = split(t)
            th[:, cols] = hi
            tl[:, cols] = lo
        for n in range(4):
            cols = slice(256 * n, 256 * n + 256)
            deep = slice(0, 256 * n + 256)
            v = dot3((th[:, deep], tl[:, deep]), (ih[cols, deep], il[cols, deep]), 1)
            hi, lo = split(v[0:512])
            vh[:, cols] = hi
            vl[:, cols] = lo
            for i in range(16):
                panel_ref[i, :, cols] = v[512 + 4 * i:516 + 4 * i]
            red_ref[:, cols] = -v[576:608]

    for n in range(4):
        @pl.when(b == n)
        def _():
            wide = slice(0, 128 * n + 128)
            for q in range(2):
                first = split(pb[0, 0, 2 * q:2 * q + 2].reshape(256, 1024))
                second = split(fb[0, 0, 2 * q:2 * q + 2].reshape(256, 1024))
                total = dot3(first, (uh[wide], ul[wide]), 1) + dot3(second, (vh[wide], vl[wide]), 1)
                for p in range(2):
                    i = 2 * q + p
                    lower = 8 * i + a >= c
                    for j in range(4):
                        at = pl.ds(j, 128, stride=4)
                        held = tr[i, at, :]
                        if j <= n:
                            new = held - total[128 * p:128 * p + 128, 128 * j:128 * j + 128]
                            held = jnp.where(lower, new, held) if j == n else new
                        out_ref[i, at, :] = held


def update(g, cm, cp, hh, pown, fown, iown, trailing):
    any_ = pl.BlockSpec(memory_space=pl.ANY)
    fixed = lambda shape: pl.BlockSpec(shape, lambda b: (0,) * len(shape), pipeline_mode=pl.Buffered(1))
    half = lambda which: pl.BlockSpec((1, 1, 4, 128, 1024), lambda b: (which, b, 0, 0, 0))
    tiles = pl.BlockSpec((4, 512, 128), lambda b: (b, 0, 0))
    return pl.pallas_call(
        update_kernel,
        grid=(4,),
        out_shape=(
            jax.ShapeDtypeStruct((32, 1024), F32),
            jax.ShapeDtypeStruct((16, 4, 1024), F32),
            jax.ShapeDtypeStruct((16, 512, 128), F32),
        ),
        in_specs=[half(0), half(1), tiles, any_, any_, any_, any_,
                  fixed((16, 4, 1024)), fixed((16, 4, 1024)), fixed((32, 1024))],
        out_specs=(
            pl.BlockSpec((32, 1024), lambda b: (0, 0)),
            pl.BlockSpec((16, 4, 1024), lambda b: (0, 0, 0)),
            tiles,
        ),
        scratch_shapes=[
            pltpu.VMEM((4, 128, 1024), F32),
            pltpu.VMEM((4, 128, 1024), F32),
            pltpu.VMEM((64, 1024), F32),
            pltpu.VMEM((2, 8, 1024, 128), F32),
            pltpu.VMEM((1024, 1024), BF16), pltpu.VMEM((1024, 1024), BF16),
            pltpu.VMEM((1024, 1024), BF16), pltpu.VMEM((1024, 1024), BF16),
            pltpu.VMEM((ROWS, 1024), BF16), pltpu.VMEM((ROWS, 1024), BF16),
            pltpu.VMEM((ROWS, 1024), BF16), pltpu.VMEM((ROWS, 1024), BF16),
            pltpu.VMEM((512, 1024), BF16), pltpu.VMEM((512, 1024), BF16),
            pltpu.SemaphoreType.DMA((3,)),
        ],
        compiler_params=pltpu.CompilerParams(
            dimension_semantics=("arbitrary",), vmem_limit_bytes=63 * 1024 * 1024
        ),
        name="update",
    )(g, g, trailing, g, cm, cp, hh, pown, fown, iown)


def body(inverse_factor, diag_block, panel_matrix, panel_factor, trailing):
    g, cm, cp, hh = gather(
        panel_matrix.reshape(4, 4, 4, 1024), panel_factor.reshape(4, 4, 4, 1024),
        inverse_factor, diag_block,
    )
    red, panel, out = update(
        g, cm, cp, hh,
        panel_matrix.reshape(16, 4, 1024), panel_factor.reshape(16, 4, 1024), inverse_factor,
        trailing.reshape(16, 512, 128),
    )
    return red, panel.reshape(panel_matrix.shape), out.reshape(trailing.shape)


def solution(mesh):
    rows = P(None, "prow", "pcol", None)
    tiles = P(None, "prow", None, None, "pcol", None)
    return jax.shard_map(
        body,
        mesh=mesh,
        in_specs=(P("pcol", None), P("pcol", None), rows, rows, tiles),
        out_specs=(P("pcol", None), rows, tiles),
        check_vma=False,
    )
```

```python
import functools

import jax
import jax.numpy as jnp
from jax import lax
from jax.experimental import pallas as pl
from jax.experimental.pallas import tpu as pltpu
from jax.sharding import PartitionSpec as P

MESH = pl.DeviceIdType.MESH
F32 = jnp.float32
BF16 = jnp.bfloat16


E_PASSES = (
    (4, ((0, 0),)),
    (5, ((1, 0), (0, 1), (0, 3))),
    (6, ((1, 3), (1, 1))),
    (7, ((0, 2), (1, 2))),
)


def comm_kernel(p_ref, f_ref, inv_ref, diag_ref, g_ref, cm_ref, cp_ref, h_ref,
                merged, swap, loc_sem, pre_send, pre_recv, xh_send, xh_recv,
                z_send, z_recv, d_send, d_recv, c_send, c_recv, cf_send, cd_send, cd_recv,
                xf_send, xf_recv, e_pre, ez_send, ez_recv, ey_send, ey_recv, ed_send, ed_recv):
    a = lax.axis_index("prow")
    c = lax.axis_index("pcol")
    xl, y = a // 4, a % 4
    z, xh, k = c // 4, (c // 2) % 2, c % 2
    d = c // 2

    partner = (a, c + 1 - 2 * k)
    z_next = (a, ((z + 1) % 8) * 4 + xh * 2 + k)
    z_prev = (a, ((z + 7) % 8) * 4 + xh * 2 + k)
    x_far = (a, z * 4 + (1 - xh) * 2 + k)
    x_near = ((1 - xl) * 4 + y, c)
    x_side = ((1 - xl) * 4 + y, z * 4 + (1 - xh) * 2 + k)
    y_next = (xl * 4 + (y + 1) % 4, c)
    y_prev = (xl * 4 + (y + 3) % 4, c)
    z_to = (z_next, z_prev)

    def remote(src, dst, send, recv, to):
        return pltpu.make_async_remote_copy(
            src_ref=src, dst_ref=dst, send_sem=send, recv_sem=recv, device_id=to, device_id_type=MESH
        )

    barrier = pltpu.get_barrier_semaphore()
    for to in (partner, z_next, z_prev, x_far, x_near, x_side, y_next, y_prev):
        pl.semaphore_signal(barrier, inc=1, device_id=to, device_id_type=MESH)
    pl.semaphore_wait(barrier, 8)

    def h_rows(which, block, start, size):
        return h_ref.at[which, block, pl.ds(pl.multiple_of(start, 32), size), :]

    def plane(h, t):
        return lax.rem(z + 8 - t, 8) if h == 0 else lax.rem(z + t, 8)

    def rows8(t, h, e):
        side = lax.rem(xh + e, 2)
        return pl.ds(pl.multiple_of(16 * plane(h, t) + 8 * side, 8), 8)

    lanes = pl.ds(pl.multiple_of(128 * a, 128), 128)
    pairs = ((p_ref, f_ref, inv_ref, diag_ref), (f_ref, p_ref, diag_ref, inv_ref))
    for me in range(2):
        @pl.when(k == me)
        def _():
            _, other, e_own, e_other = pairs[me]
            remote(
                e_other.at[:, lanes], h_rows(1 - me, a, 32 * c, 32), e_pre.at[0], e_pre.at[1], partner
            ).start()
            remote(other, swap, pre_send, pre_recv, partner).start()
            pltpu.make_async_copy(e_own.at[:, lanes], h_rows(me, a, 32 * c, 32), e_pre.at[2]).start()

    pre = remote(f_ref, swap, pre_send, pre_recv, partner)
    mine_e = pltpu.make_async_copy(inv_ref.at[:, lanes], h_rows(k, a, 32 * c, 32), e_pre.at[2])
    mine_e.wait()
    pre_e = remote(
        inv_ref.at[:, lanes], h_rows(k, a, 32 * (c + 1 - 2 * k), 32), e_pre.at[0], e_pre.at[1], partner
    )
    pre_e.wait_recv()
    far_e = remote(h_rows(k, a, 64 * d, 64), h_rows(k, a, 64 * d, 64), e_pre.at[3], e_pre.at[4], x_far)
    far_e.start()
    pre.wait_recv()
    merged[:, :, 0:4, :] = jnp.where(k == 0, p_ref[...], swap[...])
    merged[:, :, 4:8, :] = jnp.where(k == 0, swap[...], f_ref[...])

    def half(h):
        return merged.at[pl.ds(2 * h, 2)]

    def z_ref(h, t, e, j):
        return g_ref.at[k, 2 * h + j, pl.ds(0, 4 - e), rows8(t, h, e), :]

    for j in range(2):
        for h in range(2):
            remote(
                merged.at[2 * h + j], z_ref(h, 0, 0, j), z_send.at[h, 0, j, 0], z_recv.at[h, 0, j, 0], z_to[h]
            ).start()

    def far(h, e):
        ref = g_ref.at[k, pl.ds(2 * h, 2), :, rows8(0, h, e), :]
        return remote(half(h), ref, xh_send.at[h], xh_recv.at[h], x_far)

    def xf_copy(h, t, e):
        ref = g_ref.at[k, pl.ds(2 * h, 2), pl.ds(3, 1), rows8(t, h, e), :]
        return remote(ref, ref, xf_send.at[h, t], xf_recv.at[h, t], x_far)

    for h in range(2):
        far(h, 0).start()
    mine = [
        pltpu.make_async_copy(
            half(h), g_ref.at[k, pl.ds(2 * h, 2), :, rows8(0, h, 0), :], loc_sem.at[h]
        )
        for h in range(2)
    ]
    for h in range(2):
        mine[h].start()

    def z_copy(h, t, e, j):
        ref = z_ref(h, t, e, j)
        return remote(ref, ref, z_send.at[h, e, j, t], z_recv.at[h, e, j, t], z_to[h])

    def z_got(h, t, e, j):
        ref = z_ref(h, t, e, j)
        return remote(ref, ref, z_send.at[h, e, j, t - 1], z_recv.at[h, e, j, t - 1], z_to[h])

    def d_copy(h, t, e, which=None):
        ref = g_ref.at[k if which is None else which, pl.ds(2 * h, 2), :, rows8(t, h, e), :]
        return remote(ref, ref, d_send.at[h, t, e], d_recv.at[h, t, e], partner)

    def e_rows(which, dx, dy, h, t):
        block = lax.rem(xl + dx, 2) * 4 + lax.rem(y + dy, 4)
        return h_rows(which, block, 128 * plane(h, t), 128)

    def ez_copy(h, t):
        ref = e_rows(k, 0, 0, h, t)
        return remote(ref, ref, ez_send.at[h, t], ez_recv.at[h, t], z_to[h])

    def ez_got(h, t):
        ref = e_rows(k, 0, 0, h, t)
        return remote(ref, ref, ez_send.at[h, t - 1], ez_recv.at[h, t - 1], z_to[h])

    e_hops = (
        (0, 0, x_near, 1, 0),
        (0, 0, y_next, 0, 3),
        (0, 0, y_prev, 0, 1),
        (1, 0, y_next, 1, 3),
        (1, 0, y_prev, 1, 1),
        (0, 1, y_prev, 0, 2),
        (1, 3, y_next, 1, 2),
    )

    def e_copy(out, h, t):
        dx, dy, to, rx, ry = e_hops[out]
        ref = e_rows(k, dx, dy, h, t)
        return remote(ref, ref, ey_send.at[out, t + 4 * h], ey_recv.at[4 * rx + ry, t + 4 * h], to)

    def e_got(dx, dy, h, t):
        ref = e_rows(k, dx, dy, h, t)
        return remote(ref, ref, ey_send.at[0, t + 4 * h], ey_recv.at[4 * dx + dy, t + 4 * h], partner)

    def blk(dx, dy):
        return lax.rem(xl + dx, 2) * 4 + lax.rem(y + dy, 4)

    def lower(dx, dy, h, t):
        return plane(h, t) >= blk(dx, dy)

    def valid(h, t):
        return jnp.logical_and(t >= h, t <= 4 - h)

    def e_take(out_got, outs, h, t):
        dx, dy = out_got

        @pl.when(lower(dx, dy, h, t))
        def _():
            e_got(dx, dy, h, t).wait_recv()
            for out in outs:
                e_copy(out, h, t).start()

    def e_step(s):
        for h in range(2):
            @pl.when(jnp.logical_and(s <= 4 - h, lower(0, 0, h, s)))
            def _():
                ez_got(h, s).wait_recv()

                @pl.when(s < 4 - h)
                def _():
                    ez_copy(h, s).start()

                for out in range(3):
                    e_copy(out, h, s).start()

            @pl.when(valid(h, s - 1))
            def _():
                t = jnp.maximum(s - 1, h)
                e_take((1, 0), (3, 4), h, t)
                e_take((0, 1), (5,), h, t)
                e_take((0, 3), (), h, t)

            @pl.when(valid(h, s - 2))
            def _():
                t = jnp.maximum(s - 2, h)
                e_take((1, 3), (6,), h, t)
                e_take((1, 1), (), h, t)

            @pl.when(valid(h, s - 3))
            def _():
                t = jnp.maximum(s - 3, h)
                e_take((0, 2), (), h, t)
                e_take((1, 2), (), h, t)

        for at, blocks in E_PASSES:
            @pl.when(s == at)
            def _():
                e_pass_all(blocks, lambda copy: copy.start())

    def e_piece(dx, dy, p, which):
        ref = h_rows(which, blk(dx, dy), 128 * p, 128)
        return remote(ref, ref, ed_send.at[4 * dx + dy, p], ed_recv.at[4 * dx + dy, p], partner)

    def e_pass_all(blocks, act, which=None):
        def piece(p, carry):
            for dx, dy in blocks:
                @pl.when(p >= blk(dx, dy))
                def _():
                    act(e_piece(dx, dy, p, k if which is None else which))

            return carry

        lax.fori_loop(0, 8, piece, 0)

    q = z // 2
    in_plane = xl == z % 2
    y_out = (2, 1)

    def place(m):
        return lax.rem(y - (2 * xh + m) + 4, 4)

    def c_copy(m, h, t, e, out, from_g=False):
        dst = cm_ref.at[m, pl.ds(2 * h, 2), rows8(t, h, e), :]
        src = g_ref.at[k, pl.ds(2 * h, 2), q, rows8(t, h, e), :] if from_g else dst
        to = (x_near, y_next, y_prev)[out]
        return remote(src, dst, c_send.at[m, h, t, e, out], c_recv.at[m, h, t, e], to)

    def cd_copy(m, h, t, e):
        src = cm_ref.at[m, pl.ds(2 * h, 2), rows8(t, h, e), :]
        dst = cp_ref.at[pl.ds(2 * h, 2), rows8(t, h, e), :]
        return remote(src, dst, cd_send.at[h, t, e], cd_recv.at[h, t, e], partner)

    def is_source(m):
        return jnp.logical_and(in_plane, place(m) == 0)

    def off_root(m):
        return jnp.logical_and(jnp.logical_not(in_plane), place(m) == 0)

    def relays(m):
        return place(m) == (3, 1)[m]

    def is_side(m):
        return jnp.logical_and(in_plane, y == 2 * (1 - xh) + m)

    def side_copy(m, t, e):
        src = g_ref.at[k, pl.ds(2, 2), q, rows8(t, 1, e), :]
        dst = cm_ref.at[m, pl.ds(2, 2), rows8(t, 1, e), :]
        return remote(src, dst, cf_send.at[m, t, e], c_recv.at[m, 1, t, 1 - e], x_side)

    def source_sends(t, e):
        for m in range(2):
            @pl.when(is_source(m))
            def _():
                for h in range(2):
                    for out in range(h, 3):
                        c_copy(m, h, t, e, out, True).start()

            @pl.when(is_side(m))
            def _():
                side_copy(m, t, e).start()

    def take_columns(t, slot, lag):
        for m in range(2):
            r = place(m)
            when = (
                jnp.logical_or(off_root(m), jnp.logical_and(in_plane, r % 2 == 1)),
                jnp.logical_or(
                    jnp.logical_and(in_plane, r == 2),
                    jnp.logical_and(jnp.logical_not(in_plane), r % 2 == 1),
                ),
                jnp.logical_and(jnp.logical_not(in_plane), r == 2),
            )[lag - 1]

            @pl.when(jnp.logical_and(when, t >= 0))
            def _():
                s = jnp.maximum(t, 0)
                for h in range(2):
                    e = jnp.where(in_plane, slot, 1 - slot) if h == 1 else slot
                    c_copy(m, h, s, e, 0).wait_recv()

                    @pl.when(r == 0)
                    def _():
                        for out in (1, 2):
                            c_copy(m, h, s, e, out).start()

                    @pl.when(relays(m))
                    def _():
                        c_copy(m, h, s, e, y_out[m]).start()

                    @pl.when(k != m)
                    def _():
                        cd_copy(m, h, s, e).start()

    def after(t, e):
        for h in range(2):
            d_copy(h, t, e).start()
        source_sends(t, e)

    mine[0].wait()
    mine[1].wait()
    df = d + 1 - 2 * xh
    remote(
        h_rows(k, a, 64 * df, 64), h_rows(k, a, 64 * df, 64), e_pre.at[3], e_pre.at[4], x_far
    ).wait_recv()
    @pl.when(lower(0, 0, 0, 0))
    def _():
        for h in range(2):
            ez_copy(h, 0).start()
        for out in range(3):
            e_copy(out, 0, 0).start()

    after(0, 0)

    def step(s, carry):
        for j in range(2):
            for h in range(2):
                z_got(h, s, 0, j).wait_recv()

                @pl.when(s < 7)
                def _():
                    z_copy(h, s, 0, j).start()

        for h in range(2):
            xf_copy(h, s, 0).start()

        after(s, 0)
        for lag in (1, 2, 3):
            take_columns(s - lag, 0, lag)
        e_step(s)
        t = s - 1
        for h in range(2):
            @pl.when(t == 0)
            def _():
                far(h, 1).wait_recv()

        for j in range(2):
            for h in range(2):
                @pl.when(t > 0)
                def _():
                    z_got(h, jnp.maximum(t, 1), 1, j).wait_recv()

                z_copy(h, t, 1, j).start()

        for h in range(2):
            @pl.when(t > 0)
            def _():
                xf_copy(h, t, 1).wait_recv()

        after(t, 1)
        for lag in (1, 2, 3):
            take_columns(t - lag, 1, lag)
        return carry

    lax.fori_loop(1, 8, step, 0)
    last = jnp.int32(7)
    for h in range(2):
        for j in range(2):
            z_got(h, last, 1, j).wait_recv()
        xf_copy(h, last, 1).wait_recv()
    after(last, 1)
    for lag in (1, 2, 3):
        for back in range(lag, -1, -1):
            if back < lag:
                take_columns(last - back, 0, lag)
            take_columns(last - back, 1, lag)

    pre_e.wait_send()
    pre.wait_send()
    far_e.wait_send()
    for h in range(2):
        far(h, 0).wait_send()
        for t in range(5 - h):
            if t < 4 - h:
                @pl.when(lower(0, 0, h, t))
                def _():
                    ez_copy(h, t).wait_send()

            if t >= h:
                for out in range(7):
                    @pl.when(lower(*e_hops[out][:2], h, t))
                    def _():
                        e_copy(out, h, t).wait_send()

    for _, blocks in E_PASSES:
        e_pass_all(blocks, lambda copy: copy.wait_send())
        e_pass_all(blocks, lambda copy: copy.wait_recv(), 1 - k)

    def finish(t, carry):
        for e in range(2):
            for h in range(2):
                @pl.when(t < 7)
                def _():
                    for j in range(2):
                        z_copy(h, t, e, j).wait_send()

                if e == 0:
                    @pl.when(t > 0)
                    def _():
                        xf_copy(h, t, 0).wait_send()

                d_copy(h, t, e).wait_send()
                d_copy(h, t, e, 1 - k).wait_recv()
                for m in range(2):
                    if h == 1:
                        @pl.when(is_side(m))
                        def _():
                            side_copy(m, t, e).wait_send()

                    @pl.when(is_source(m))
                    def _():
                        for out in range(h, 3):
                            c_copy(m, h, t, e, out, True).wait_send()

                    @pl.when(off_root(m))
                    def _():
                        for out in (1, 2):
                            c_copy(m, h, t, e, out).wait_send()

                    @pl.when(relays(m))
                    def _():
                        c_copy(m, h, t, e, y_out[m]).wait_send()

                    @pl.when(jnp.logical_not(is_source(m)))
                    def _():
                        @pl.when(k != m)
                        def _():
                            cd_copy(m, h, t, e).wait_send()

                        @pl.when(k == m)
                        def _():
                            cd_copy(m, h, t, e).wait_recv()

        return carry

    lax.fori_loop(0, 8, finish, 0)


def gather(p4, f4, inverse_factor, diag_block):
    dma = pltpu.SemaphoreType.DMA
    return pl.pallas_call(
        comm_kernel,
        out_shape=(
            jax.ShapeDtypeStruct((2, 4, 4, 128, 1024), F32),
            jax.ShapeDtypeStruct((2, 4, 128, 1024), F32),
            jax.ShapeDtypeStruct((4, 128, 1024), F32),
            jax.ShapeDtypeStruct((2, 8, 1024, 128), F32),
        ),
        in_specs=[pl.BlockSpec(memory_space=pltpu.VMEM)] * 4,
        out_specs=(pl.BlockSpec(memory_space=pl.ANY),) * 4,
        scratch_shapes=[
            pltpu.VMEM((4, 4, 8, 1024), F32),
            pltpu.VMEM((4, 4, 4, 1024), F32),
            dma((2,)), dma, dma, dma((2,)), dma((2,)),
            dma((2, 2, 2, 7)), dma((2, 2, 2, 7)),
            dma((2, 8, 2)), dma((2, 8, 2)),
            dma((2, 2, 8, 2, 3)), dma((2, 2, 8, 2)), dma((2, 8, 2)),
            dma((2, 8, 2)), dma((2, 8, 2)),
            dma((2, 8)), dma((2, 8)),
            dma((5,)),
            dma((2, 4)), dma((2, 4)),
            dma((7, 8)), dma((8, 8)),
            dma((8, 8)), dma((8, 8)),
        ],
        compiler_params=pltpu.CompilerParams(collective_id=0, has_side_effects=True),
        name="gather",
    )(p4, f4, inverse_factor, diag_block)


def split(v):
    hi = v.astype(BF16)
    return hi, (v - hi.astype(F32)).astype(BF16)


def dot3(x, y, contract):
    (xh, xlo), (yh, ylo) = x, y
    dims = (((1,), (contract,)), ((), ()))
    dot = functools.partial(lax.dot_general, dimension_numbers=dims, preferred_element_type=F32)
    return dot(xh, yh) + dot(xlo, yh) + dot(xh, ylo)


ROWS = 608


def update_kernel(tr, g_ref, cm_ref, cp_ref, h_ref, pown, fown, iown,
                  red_ref, panel_ref, out_ref,
                  pb, fb, pc, fc, po, hv, ih, il, dh, dl, uh, ul, th, tl, vh, vl, sems):
    b = pl.program_id(0)
    a = lax.axis_index("prow")
    c = lax.axis_index("pcol")
    z, xh, k = c // 4, (c // 2) % 2, c % 2
    source = a == (z % 2) * 4 + 2 * xh + k

    def stream(n):
        return [
            pltpu.make_async_copy(g_ref.at[w, n], (pb, fb)[w].at[n % 2], sems.at[2 + 2 * w + n % 2])
            for w in range(2)
        ]

    def slices(g):
        deep = pl.ds(128 * g, 1024 - 128 * g)
        return [
            pltpu.make_async_copy(h_ref.at[w, g, deep], hv.at[w, g, deep], sems.at[6 + 8 * w + g])
            for w in range(2)
        ]

    @pl.when(b == 0)
    def _():
        for g in range(8):
            for copy in slices(g):
                copy.start()

        @pl.when(source)
        def _():
            pltpu.make_async_copy(g_ref.at[0, :, z // 2], pc, sems.at[0]).start()
            pltpu.make_async_copy(g_ref.at[1, :, z // 2], fc, sems.at[1]).start()

        @pl.when(jnp.logical_not(source))
        def _():
            @pl.when(k == 0)
            def _():
                pltpu.make_async_copy(cm_ref.at[0], pc, sems.at[0]).start()
                pltpu.make_async_copy(cp_ref, fc, sems.at[1]).start()

            @pl.when(k == 1)
            def _():
                pltpu.make_async_copy(cp_ref, pc, sems.at[0]).start()
                pltpu.make_async_copy(cm_ref.at[1], fc, sems.at[1]).start()

        for n in range(2):
            for copy in stream(n):
                copy.start()
        for g in range(8):
            lanes = slice(128 * g, 128 * g + 128)
            deep = slice(128 * g, 1024)
            for copy in slices(g):
                copy.wait()
            hi, lo = split(hv[0, g, deep])
            ih[deep, lanes] = hi
            il[deep, lanes] = lo
            hi, lo = split(hv[1, g, deep])
            dh[deep, lanes] = hi
            dl[deep, lanes] = lo
            if g % 2 == 1:
                top = slice(128 * g - 128, 128 * g)
                ih[top, lanes] = jnp.zeros((128, 128), BF16)
                il[top, lanes] = jnp.zeros((128, 128), BF16)
            for r in range(g + 1, 8):
                rows = slice(128 * r, 128 * r + 128)
                hi, lo = split(hv[1, g, rows].T)
                dh[lanes, rows] = hi
                dl[lanes, rows] = lo
        pltpu.make_async_copy(cm_ref.at[0], pc, sems.at[0]).wait()
        pltpu.make_async_copy(cm_ref.at[0], fc, sems.at[1]).wait()

        hi, lo = split(fc[...].reshape(512, 1024))
        th[0:512] = hi
        tl[0:512] = lo
        for i in range(16):
            po[4 * i:4 * i + 4] = fown[i]
        hi, lo = split(po[...])
        th[512:576] = hi
        tl[512:576] = lo
        for i in range(16):
            po[4 * i:4 * i + 4] = pown[i]
        for n in range(4):
            cols = slice(256 * n, 256 * n + 256)
            deep = slice(256 * n, 1024)
            u = dot3(
                (th[0:576, deep], tl[0:576, deep]), (ih[deep, cols], il[deep, cols]), 0
            )
            hi, lo = split(u)
            uh[0:576, cols] = hi
            ul[0:576, cols] = lo
        hi, lo = split(iown[...])
        uh[576:608] = hi
        ul[576:608] = lo
        for n in range(4):
            cols = slice(256 * n, 256 * n + 256)
            start = jnp.concatenate(
                [pc[:, :, cols].reshape(512, 256), po[:, cols], jnp.zeros((32, 256), F32)]
            )
            t = start - dot3((uh[...], ul[...]), (dh[:, cols], dl[:, cols]), 0)
            hi, lo = split(t)
            th[:, cols] = hi
            tl[:, cols] = lo
        for n in range(4):
            cols = slice(256 * n, 256 * n + 256)
            deep = slice(0, 256 * n + 256)
            v = dot3((th[:, deep], tl[:, deep]), (ih[cols, deep], il[cols, deep]), 1)
            hi, lo = split(v[0:512])
            vh[:, cols] = hi
            vl[:, cols] = lo
            for i in range(16):
                panel_ref[i, :, cols] = v[512 + 4 * i:516 + 4 * i]
            red_ref[:, cols] = -v[576:608]

    for n in range(4):
        @pl.when(b == n)
        def _():
            if 0 < n < 3:
                for copy in stream(n + 1):
                    copy.start()
            for copy in stream(n):
                copy.wait()
            wide = slice(0, 128 * n + 128)
            for q in range(2):
                first = split(pb[n % 2, 2 * q:2 * q + 2].reshape(256, 1024))
                second = split(fb[n % 2, 2 * q:2 * q + 2].reshape(256, 1024))
                total = dot3(first, (uh[wide], ul[wide]), 1) + dot3(second, (vh[wide], vl[wide]), 1)
                for p in range(2):
                    i = 2 * q + p
                    lower = 8 * i + a >= c
                    for j in range(4):
                        at = pl.ds(j, 128, stride=4)
                        held = tr[i, at, :]
                        if j <= n:
                            new = held - total[128 * p:128 * p + 128, 128 * j:128 * j + 128]
                            held = jnp.where(lower, new, held) if j == n else new
                        out_ref[i, at, :] = held


def update(g, cm, cp, hh, pown, fown, iown, trailing):
    any_ = pl.BlockSpec(memory_space=pl.ANY)
    fixed = lambda shape: pl.BlockSpec(shape, lambda b: (0,) * len(shape), pipeline_mode=pl.Buffered(1))
    tiles = pl.BlockSpec((4, 512, 128), lambda b: (b, 0, 0))
    return pl.pallas_call(
        update_kernel,
        grid=(4,),
        out_shape=(
            jax.ShapeDtypeStruct((32, 1024), F32),
            jax.ShapeDtypeStruct((16, 4, 1024), F32),
            jax.ShapeDtypeStruct((16, 512, 128), F32),
        ),
        in_specs=[tiles, any_, any_, any_, any_,
                  fixed((16, 4, 1024)), fixed((16, 4, 1024)), fixed((32, 1024))],
        out_specs=(
            pl.BlockSpec((32, 1024), lambda b: (0, 0)),
            pl.BlockSpec((16, 4, 1024), lambda b: (0, 0, 0)),
            tiles,
        ),
        scratch_shapes=[
            pltpu.VMEM((2, 4, 128, 1024), F32),
            pltpu.VMEM((2, 4, 128, 1024), F32),
            pltpu.VMEM((4, 128, 1024), F32),
            pltpu.VMEM((4, 128, 1024), F32),
            pltpu.VMEM((64, 1024), F32),
            pltpu.VMEM((2, 8, 1024, 128), F32),
            pltpu.VMEM((1024, 1024), BF16), pltpu.VMEM((1024, 1024), BF16),
            pltpu.VMEM((1024, 1024), BF16), pltpu.VMEM((1024, 1024), BF16),
            pltpu.VMEM((ROWS, 1024), BF16), pltpu.VMEM((ROWS, 1024), BF16),
            pltpu.VMEM((ROWS, 1024), BF16), pltpu.VMEM((ROWS, 1024), BF16),
            pltpu.VMEM((512, 1024), BF16), pltpu.VMEM((512, 1024), BF16),
            pltpu.SemaphoreType.DMA((22,)),
        ],
        compiler_params=pltpu.CompilerParams(
            dimension_semantics=("arbitrary",), vmem_limit_bytes=63 * 1024 * 1024
        ),
        name="update",
    )(trailing, g, cm, cp, hh, pown, fown, iown)


def body(inverse_factor, diag_block, panel_matrix, panel_factor, trailing):
    g, cm, cp, hh = gather(
        panel_matrix.reshape(4, 4, 4, 1024), panel_factor.reshape(4, 4, 4, 1024),
        inverse_factor, diag_block,
    )
    red, panel, out = update(
        g, cm, cp, hh,
        panel_matrix.reshape(16, 4, 1024), panel_factor.reshape(16, 4, 1024), inverse_factor,
        trailing.reshape(16, 512, 128),
    )
    return red, panel.reshape(panel_matrix.shape), out.reshape(trailing.shape)


def solution(mesh):
    rows = P(None, "prow", "pcol", None)
    tiles = P(None, "prow", None, None, "pcol", None)
    return jax.shard_map(
        body,
        mesh=mesh,
        in_specs=(P("pcol", None), P("pcol", None), rows, rows, tiles),
        out_specs=(P("pcol", None), rows, tiles),
        check_vma=False,
    )
```

```python
import functools

import jax
import jax.numpy as jnp
from jax import lax
from jax.experimental import pallas as pl
from jax.experimental.pallas import tpu as pltpu
from jax.sharding import PartitionSpec as P

MESH = pl.DeviceIdType.MESH
F32 = jnp.float32
BF16 = jnp.bfloat16


E_PASSES = (
    (4, ((0, 0),)),
    (5, ((1, 0), (0, 1), (0, 3))),
    (6, ((1, 3), (1, 1))),
    (7, ((0, 2), (1, 2))),
)


def comm_kernel(p_ref, f_ref, inv_ref, diag_ref, g_ref, cm_ref, cp_ref, h_ref,
                merged, swap, loc_sem, pre_send, pre_recv, xh_send, xh_recv,
                z_send, z_recv, d_send, d_recv, c_send, c_recv, cf_send, cd_send, cd_recv,
                xf_send, xf_recv, e_pre, ez_send, ez_recv, ey_send, ey_recv, ed_send, ed_recv):
    a = lax.axis_index("prow")
    c = lax.axis_index("pcol")
    xl, y = a // 4, a % 4
    z, xh, k = c // 4, (c // 2) % 2, c % 2
    d = c // 2

    partner = (a, c + 1 - 2 * k)
    z_next = (a, ((z + 1) % 8) * 4 + xh * 2 + k)
    z_prev = (a, ((z + 7) % 8) * 4 + xh * 2 + k)
    x_far = (a, z * 4 + (1 - xh) * 2 + k)
    x_near = ((1 - xl) * 4 + y, c)
    x_side = ((1 - xl) * 4 + y, z * 4 + (1 - xh) * 2 + k)
    y_next = (xl * 4 + (y + 1) % 4, c)
    y_prev = (xl * 4 + (y + 3) % 4, c)
    z_to = (z_next, z_prev)

    def remote(src, dst, send, recv, to):
        return pltpu.make_async_remote_copy(
            src_ref=src, dst_ref=dst, send_sem=send, recv_sem=recv, device_id=to, device_id_type=MESH
        )

    barrier = pltpu.get_barrier_semaphore()
    for to in (partner, z_next, z_prev, x_far, x_near, x_side, y_next, y_prev):
        pl.semaphore_signal(barrier, inc=1, device_id=to, device_id_type=MESH)
    pl.semaphore_wait(barrier, 8)

    def h_rows(which, block, start, size):
        return h_ref.at[which, block, pl.ds(pl.multiple_of(start, 32), size), :]

    def plane(h, t):
        return lax.rem(z + 8 - t, 8) if h == 0 else lax.rem(z + t, 8)

    def rows8(t, h, e):
        side = lax.rem(xh + e, 2)
        return pl.ds(pl.multiple_of(16 * plane(h, t) + 8 * side, 8), 8)

    lanes = pl.ds(pl.multiple_of(128 * a, 128), 128)
    pairs = ((p_ref, f_ref, inv_ref, diag_ref), (f_ref, p_ref, diag_ref, inv_ref))
    for me in range(2):
        @pl.when(k == me)
        def _():
            _, other, e_own, e_other = pairs[me]
            remote(
                e_other.at[:, lanes], h_rows(1 - me, a, 32 * c, 32), e_pre.at[0], e_pre.at[1], partner
            ).start()
            remote(other, swap, pre_send, pre_recv, partner).start()
            pltpu.make_async_copy(e_own.at[:, lanes], h_rows(me, a, 32 * c, 32), e_pre.at[2]).start()

    pre = remote(f_ref, swap, pre_send, pre_recv, partner)
    mine_e = pltpu.make_async_copy(inv_ref.at[:, lanes], h_rows(k, a, 32 * c, 32), e_pre.at[2])
    mine_e.wait()
    pre_e = remote(
        inv_ref.at[:, lanes], h_rows(k, a, 32 * (c + 1 - 2 * k), 32), e_pre.at[0], e_pre.at[1], partner
    )
    pre_e.wait_recv()
    far_e = remote(h_rows(k, a, 64 * d, 64), h_rows(k, a, 64 * d, 64), e_pre.at[3], e_pre.at[4], x_far)
    far_e.start()
    pre.wait_recv()
    merged[:, :, 0:4, :] = jnp.where(k == 0, p_ref[...], swap[...])
    merged[:, :, 4:8, :] = jnp.where(k == 0, swap[...], f_ref[...])

    def half(h):
        return merged.at[pl.ds(2 * h, 2)]

    def z_ref(h, t, e, j):
        return g_ref.at[k, 2 * h + j, pl.ds(0, 4 - e), rows8(t, h, e), :]

    for j in range(2):
        for h in range(2):
            remote(
                merged.at[2 * h + j], z_ref(h, 0, 0, j), z_send.at[0], z_recv.at[h, 0, j, 0], z_to[h]
            ).start()

    def far(h, e):
        ref = g_ref.at[k, pl.ds(2 * h, 2), :, rows8(0, h, e), :]
        return remote(half(h), ref, xh_send.at[h], xh_recv.at[h], x_far)

    def xf_copy(h, t, e):
        ref = g_ref.at[k, pl.ds(2 * h, 2), pl.ds(3, 1), rows8(t, h, e), :]
        return remote(ref, ref, xf_send, xf_recv.at[h, t], x_far)

    for h in range(2):
        far(h, 0).start()
    mine = [
        pltpu.make_async_copy(
            half(h), g_ref.at[k, pl.ds(2 * h, 2), :, rows8(0, h, 0), :], loc_sem.at[h]
        )
        for h in range(2)
    ]
    for h in range(2):
        mine[h].start()

    def z_copy(h, t, e, j):
        ref = z_ref(h, t, e, j)
        return remote(ref, ref, z_send.at[e], z_recv.at[h, e, j, t], z_to[h])

    def z_got(h, t, e, j):
        ref = z_ref(h, t, e, j)
        return remote(ref, ref, z_send.at[e], z_recv.at[h, e, j, t - 1], z_to[h])

    def d_copy(h, t, e, which=None):
        ref = g_ref.at[k if which is None else which, pl.ds(2 * h, 2), :, rows8(t, h, e), :]
        return remote(ref, ref, d_send, d_recv, partner)

    def e_rows(which, dx, dy, h, t):
        block = lax.rem(xl + dx, 2) * 4 + lax.rem(y + dy, 4)
        return h_rows(which, block, 128 * plane(h, t), 128)

    def ez_copy(h, t):
        ref = e_rows(k, 0, 0, h, t)
        return remote(ref, ref, ez_send.at[h, t], ez_recv.at[h, t], z_to[h])

    def ez_got(h, t):
        ref = e_rows(k, 0, 0, h, t)
        return remote(ref, ref, ez_send.at[h, t - 1], ez_recv.at[h, t - 1], z_to[h])

    e_hops = (
        (0, 0, x_near, 1, 0),
        (0, 0, y_next, 0, 3),
        (0, 0, y_prev, 0, 1),
        (1, 0, y_next, 1, 3),
        (1, 0, y_prev, 1, 1),
        (0, 1, y_prev, 0, 2),
        (1, 3, y_next, 1, 2),
    )

    def e_copy(out, h, t):
        dx, dy, to, rx, ry = e_hops[out]
        ref = e_rows(k, dx, dy, h, t)
        return remote(ref, ref, ey_send.at[out, t + 4 * h], ey_recv.at[4 * rx + ry, t + 4 * h], to)

    def e_got(dx, dy, h, t):
        ref = e_rows(k, dx, dy, h, t)
        return remote(ref, ref, ey_send.at[0, t + 4 * h], ey_recv.at[4 * dx + dy, t + 4 * h], partner)

    def blk(dx, dy):
        return lax.rem(xl + dx, 2) * 4 + lax.rem(y + dy, 4)

    def lower(dx, dy, h, t):
        return plane(h, t) >= blk(dx, dy)

    def valid(h, t):
        return jnp.logical_and(t >= h, t <= 4 - h)

    def e_take(out_got, outs, h, t):
        dx, dy = out_got

        @pl.when(lower(dx, dy, h, t))
        def _():
            e_got(dx, dy, h, t).wait_recv()
            for out in outs:
                e_copy(out, h, t).start()

    def e_step(s):
        for h in range(2):
            @pl.when(jnp.logical_and(s <= 4 - h, lower(0, 0, h, s)))
            def _():
                ez_got(h, s).wait_recv()

                @pl.when(s < 4 - h)
                def _():
                    ez_copy(h, s).start()

                for out in range(3):
                    e_copy(out, h, s).start()

            @pl.when(valid(h, s - 1))
            def _():
                t = jnp.maximum(s - 1, h)
                e_take((1, 0), (3, 4), h, t)
                e_take((0, 1), (5,), h, t)
                e_take((0, 3), (), h, t)

            @pl.when(valid(h, s - 2))
            def _():
                t = jnp.maximum(s - 2, h)
                e_take((1, 3), (6,), h, t)
                e_take((1, 1), (), h, t)

            @pl.when(valid(h, s - 3))
            def _():
                t = jnp.maximum(s - 3, h)
                e_take((0, 2), (), h, t)
                e_take((1, 2), (), h, t)

        for at, blocks in E_PASSES:
            @pl.when(s == at)
            def _():
                e_pass_all(blocks, lambda copy: copy.start())

    def e_piece(dx, dy, p, which):
        ref = h_rows(which, blk(dx, dy), 128 * p, 128)
        return remote(ref, ref, ed_send.at[4 * dx + dy, p], ed_recv.at[4 * dx + dy, p], partner)

    def e_pass_all(blocks, act, which=None):
        def piece(p, carry):
            for dx, dy in blocks:
                @pl.when(p >= blk(dx, dy))
                def _():
                    act(e_piece(dx, dy, p, k if which is None else which))

            return carry

        lax.fori_loop(0, 8, piece, 0)

    q = z // 2
    in_plane = xl == z % 2
    y_out = (2, 1)

    def place(m):
        return lax.rem(y - (2 * xh + m) + 4, 4)

    def c_copy(m, h, t, e, out, from_g=False):
        dst = cm_ref.at[m, pl.ds(2 * h, 2), rows8(t, h, e), :]
        src = g_ref.at[k, pl.ds(2 * h, 2), q, rows8(t, h, e), :] if from_g else dst
        to = (x_near, y_next, y_prev)[out]
        return remote(src, dst, c_send.at[m, out], c_recv.at[m, h, t, e], to)

    def cd_copy(m, h, t, e):
        src = cm_ref.at[m, pl.ds(2 * h, 2), rows8(t, h, e), :]
        dst = cp_ref.at[pl.ds(2 * h, 2), rows8(t, h, e), :]
        return remote(src, dst, cd_send, cd_recv, partner)

    def is_source(m):
        return jnp.logical_and(in_plane, place(m) == 0)

    def off_root(m):
        return jnp.logical_and(jnp.logical_not(in_plane), place(m) == 0)

    def relays(m):
        return place(m) == (3, 1)[m]

    def is_side(m):
        return jnp.logical_and(in_plane, y == 2 * (1 - xh) + m)

    def side_copy(m, t, e):
        src = g_ref.at[k, pl.ds(2, 2), q, rows8(t, 1, e), :]
        dst = cm_ref.at[m, pl.ds(2, 2), rows8(t, 1, e), :]
        return remote(src, dst, cf_send.at[m], c_recv.at[m, 1, t, 1 - e], x_side)

    def source_sends(t, e):
        for m in range(2):
            @pl.when(is_source(m))
            def _():
                for h in range(2):
                    for out in range(h, 3):
                        c_copy(m, h, t, e, out, True).start()

            @pl.when(is_side(m))
            def _():
                side_copy(m, t, e).start()

    def take_columns(t, slot, lag):
        for m in range(2):
            r = place(m)
            when = (
                jnp.logical_or(off_root(m), jnp.logical_and(in_plane, r % 2 == 1)),
                jnp.logical_or(
                    jnp.logical_and(in_plane, r == 2),
                    jnp.logical_and(jnp.logical_not(in_plane), r % 2 == 1),
                ),
                jnp.logical_and(jnp.logical_not(in_plane), r == 2),
            )[lag - 1]

            @pl.when(jnp.logical_and(when, t >= 0))
            def _():
                s = jnp.maximum(t, 0)
                for h in range(2):
                    e = jnp.where(in_plane, slot, 1 - slot) if h == 1 else slot
                    c_copy(m, h, s, e, 0).wait_recv()

                    @pl.when(r == 0)
                    def _():
                        for out in (1, 2):
                            c_copy(m, h, s, e, out).start()

                    @pl.when(relays(m))
                    def _():
                        c_copy(m, h, s, e, y_out[m]).start()

                    @pl.when(k != m)
                    def _():
                        cd_copy(m, h, s, e).start()

    def after(t, e):
        source_sends(t, e)
        for h in range(2):
            d_copy(h, t, e).start()

    mine[0].wait()
    mine[1].wait()
    df = d + 1 - 2 * xh
    remote(
        h_rows(k, a, 64 * df, 64), h_rows(k, a, 64 * df, 64), e_pre.at[3], e_pre.at[4], x_far
    ).wait_recv()
    @pl.when(lower(0, 0, 0, 0))
    def _():
        for h in range(2):
            ez_copy(h, 0).start()
        for out in range(3):
            e_copy(out, 0, 0).start()

    after(0, 0)

    def step(s, carry):
        for j in range(2):
            for h in range(2):
                z_got(h, s, 0, j).wait_recv()

                @pl.when(s < 7)
                def _():
                    z_copy(h, s, 0, j).start()

        for h in range(2):
            xf_copy(h, s, 0).start()

        after(s, 0)
        for lag in (1, 2, 3):
            take_columns(s - lag, 0, lag)
        e_step(s)
        t = s - 1
        for h in range(2):
            @pl.when(t == 0)
            def _():
                far(h, 1).wait_recv()

        for j in range(2):
            for h in range(2):
                @pl.when(t > 0)
                def _():
                    z_got(h, jnp.maximum(t, 1), 1, j).wait_recv()

                z_copy(h, t, 1, j).start()

        for h in range(2):
            @pl.when(t > 0)
            def _():
                xf_copy(h, t, 1).wait_recv()

        after(t, 1)
        for lag in (1, 2, 3):
            take_columns(t - lag, 1, lag)
        return carry

    lax.fori_loop(1, 8, step, 0)
    last = jnp.int32(7)
    for h in range(2):
        for j in range(2):
            z_got(h, last, 1, j).wait_recv()
        xf_copy(h, last, 1).wait_recv()
    after(last, 1)
    for lag in (1, 2, 3):
        for back in range(lag, -1, -1):
            if back < lag:
                take_columns(last - back, 0, lag)
            take_columns(last - back, 1, lag)

    pre_e.wait_send()
    pre.wait_send()
    far_e.wait_send()
    for h in range(2):
        far(h, 0).wait_send()
        for t in range(5 - h):
            if t < 4 - h:
                @pl.when(lower(0, 0, h, t))
                def _():
                    ez_copy(h, t).wait_send()

            if t >= h:
                for out in range(7):
                    @pl.when(lower(*e_hops[out][:2], h, t))
                    def _():
                        e_copy(out, h, t).wait_send()

    for _, blocks in E_PASSES:
        e_pass_all(blocks, lambda copy: copy.wait_send())
        e_pass_all(blocks, lambda copy: copy.wait_recv(), 1 - k)

    def sent(ref, sem):
        remote(ref, ref, sem, xh_recv.at[0], partner).wait_send()

    steps = pl.ds(0, 112)
    sent(g_ref.at[k, pl.ds(0, 2), :, steps, :], z_send.at[0])
    sent(g_ref.at[k, pl.ds(0, 2), pl.ds(0, 3), steps, :], z_send.at[1])
    sent(g_ref.at[k, pl.ds(0, 2), pl.ds(0, 1), steps, :], xf_send)
    for m in range(2):
        whole, part = cm_ref.at[m], cm_ref.at[m, pl.ds(0, 2)]

        @pl.when(is_side(m))
        def _():
            sent(part, cf_send.at[m])

        @pl.when(is_source(m))
        def _():
            sent(part, c_send.at[m, 0])

        @pl.when(place(m) == 0)
        def _():
            for out in (1, 2):
                sent(whole, c_send.at[m, out])

        @pl.when(relays(m))
        def _():
            sent(whole, c_send.at[m, y_out[m]])

        @pl.when(jnp.logical_not(is_source(m)))
        def _():
            @pl.when(k != m)
            def _():
                sent(cp_ref, cd_send)

            @pl.when(k == m)
            def _():
                remote(cp_ref, cp_ref, cd_send, cd_recv, partner).wait_recv()

    sent(g_ref.at[k], d_send)
    remote(g_ref.at[1 - k], g_ref.at[1 - k], d_send, d_recv, partner).wait_recv()


def gather(p4, f4, inverse_factor, diag_block):
    dma = pltpu.SemaphoreType.DMA
    return pl.pallas_call(
        comm_kernel,
        out_shape=(
            jax.ShapeDtypeStruct((2, 4, 4, 128, 1024), F32),
            jax.ShapeDtypeStruct((2, 4, 128, 1024), F32),
            jax.ShapeDtypeStruct((4, 128, 1024), F32),
            jax.ShapeDtypeStruct((2, 8, 1024, 128), F32),
        ),
        in_specs=[pl.BlockSpec(memory_space=pltpu.VMEM)] * 4,
        out_specs=(pl.BlockSpec(memory_space=pl.ANY),) * 4,
        scratch_shapes=[
            pltpu.VMEM((4, 4, 8, 1024), F32),
            pltpu.VMEM((4, 4, 4, 1024), F32),
            dma((2,)), dma, dma, dma((2,)), dma((2,)),
            dma((2,)), dma((2, 2, 2, 7)),
            dma, dma,
            dma((2, 3)), dma((2, 2, 8, 2)), dma((2,)),
            dma, dma,
            dma, dma((2, 8)),
            dma((5,)),
            dma((2, 4)), dma((2, 4)),
            dma((7, 8)), dma((8, 8)),
            dma((8, 8)), dma((8, 8)),
        ],
        compiler_params=pltpu.CompilerParams(collective_id=0, has_side_effects=True),
        name="gather",
    )(p4, f4, inverse_factor, diag_block)


def split(v):
    hi = v.astype(BF16)
    return hi, (v - hi.astype(F32)).astype(BF16)


def dot3(x, y, contract):
    (xh, xlo), (yh, ylo) = x, y
    dims = (((1,), (contract,)), ((), ()))
    dot = functools.partial(lax.dot_general, dimension_numbers=dims, preferred_element_type=F32)
    return dot(xh, yh) + dot(xlo, yh) + dot(xh, ylo)


ROWS = 608


def update_kernel(tr, g_ref, cm_ref, cp_ref, h_ref, pown, fown, iown,
                  red_ref, panel_ref, out_ref,
                  pb, fb, pc, fc, po, hv, ih, il, dh, dl, uh, ul, th, tl, vh, vl, sems):
    b = pl.program_id(0)
    a = lax.axis_index("prow")
    c = lax.axis_index("pcol")
    z, xh, k = c // 4, (c // 2) % 2, c % 2
    source = a == (z % 2) * 4 + 2 * xh + k

    def stream(n):
        return [
            pltpu.make_async_copy(g_ref.at[w, n], (pb, fb)[w].at[n % 2], sems.at[2 + 2 * w + n % 2])
            for w in range(2)
        ]

    def slices(g):
        deep = pl.ds(128 * g, 1024 - 128 * g)
        return [
            pltpu.make_async_copy(h_ref.at[w, g, deep], hv.at[w, g, deep], sems.at[6 + 8 * w + g])
            for w in range(2)
        ]

    @pl.when(b == 0)
    def _():
        for g in range(8):
            for copy in slices(g):
                copy.start()

        @pl.when(source)
        def _():
            pltpu.make_async_copy(g_ref.at[0, :, z // 2], pc, sems.at[0]).start()
            pltpu.make_async_copy(g_ref.at[1, :, z // 2], fc, sems.at[1]).start()

        @pl.when(jnp.logical_not(source))
        def _():
            @pl.when(k == 0)
            def _():
                pltpu.make_async_copy(cm_ref.at[0], pc, sems.at[0]).start()
                pltpu.make_async_copy(cp_ref, fc, sems.at[1]).start()

            @pl.when(k == 1)
            def _():
                pltpu.make_async_copy(cp_ref, pc, sems.at[0]).start()
                pltpu.make_async_copy(cm_ref.at[1], fc, sems.at[1]).start()

        for n in range(2):
            for copy in stream(n):
                copy.start()
        for g in range(8):
            lanes = slice(128 * g, 128 * g + 128)
            deep = slice(128 * g, 1024)
            for copy in slices(g):
                copy.wait()
            hi, lo = split(hv[0, g, deep])
            ih[deep, lanes] = hi
            il[deep, lanes] = lo
            hi, lo = split(hv[1, g, deep])
            dh[deep, lanes] = hi
            dl[deep, lanes] = lo
            if g % 2 == 1:
                top = slice(128 * g - 128, 128 * g)
                ih[top, lanes] = jnp.zeros((128, 128), BF16)
                il[top, lanes] = jnp.zeros((128, 128), BF16)
            for r in range(g + 1, 8):
                rows = slice(128 * r, 128 * r + 128)
                hi, lo = split(hv[1, g, rows].T)
                dh[lanes, rows] = hi
                dl[lanes, rows] = lo
        pltpu.make_async_copy(cm_ref.at[0], pc, sems.at[0]).wait()
        pltpu.make_async_copy(cm_ref.at[0], fc, sems.at[1]).wait()

        hi, lo = split(fc[...].reshape(512, 1024))
        th[0:512] = hi
        tl[0:512] = lo
        for i in range(16):
            po[4 * i:4 * i + 4] = fown[i]
        hi, lo = split(po[...])
        th[512:576] = hi
        tl[512:576] = lo
        for i in range(16):
            po[4 * i:4 * i + 4] = pown[i]
        for n in range(4):
            cols = slice(256 * n, 256 * n + 256)
            deep = slice(256 * n, 1024)
            u = dot3(
                (th[0:576, deep], tl[0:576, deep]), (ih[deep, cols], il[deep, cols]), 0
            )
            hi, lo = split(u)
            uh[0:576, cols] = hi
            ul[0:576, cols] = lo
        hi, lo = split(iown[...])
        uh[576:608] = hi
        ul[576:608] = lo
        for n in range(4):
            cols = slice(256 * n, 256 * n + 256)
            start = jnp.concatenate(
                [pc[:, :, cols].reshape(512, 256), po[:, cols], jnp.zeros((32, 256), F32)]
            )
            t = start - dot3((uh[...], ul[...]), (dh[:, cols], dl[:, cols]), 0)
            hi, lo = split(t)
            th[:, cols] = hi
            tl[:, cols] = lo
        for n in range(4):
            cols = slice(256 * n, 256 * n + 256)
            deep = slice(0, 256 * n + 256)
            v = dot3((th[:, deep], tl[:, deep]), (ih[cols, deep], il[cols, deep]), 1)
            hi, lo = split(v[0:512])
            vh[:, cols] = hi
            vl[:, cols] = lo
            for i in range(16):
                panel_ref[i, :, cols] = v[512 + 4 * i:516 + 4 * i]
            red_ref[:, cols] = -v[576:608]

    for n in range(4):
        @pl.when(b == n)
        def _():
            if 0 < n < 3:
                for copy in stream(n + 1):
                    copy.start()
            for copy in stream(n):
                copy.wait()
            wide = slice(0, 128 * n + 128)
            for q in range(2):
                first = split(pb[n % 2, 2 * q:2 * q + 2].reshape(256, 1024))
                second = split(fb[n % 2, 2 * q:2 * q + 2].reshape(256, 1024))
                total = dot3(first, (uh[wide], ul[wide]), 1) + dot3(second, (vh[wide], vl[wide]), 1)
                for p in range(2):
                    i = 2 * q + p
                    lower = 8 * i + a >= c
                    for j in range(4):
                        at = pl.ds(j, 128, stride=4)
                        held = tr[i, at, :]
                        if j <= n:
                            new = held - total[128 * p:128 * p + 128, 128 * j:128 * j + 128]
                            held = jnp.where(lower, new, held) if j == n else new
                        out_ref[i, at, :] = held


def update(g, cm, cp, hh, pown, fown, iown, trailing):
    any_ = pl.BlockSpec(memory_space=pl.ANY)
    fixed = lambda shape: pl.BlockSpec(shape, lambda b: (0,) * len(shape), pipeline_mode=pl.Buffered(1))
    tiles = pl.BlockSpec((4, 512, 128), lambda b: (b, 0, 0))
    return pl.pallas_call(
        update_kernel,
        grid=(4,),
        out_shape=(
            jax.ShapeDtypeStruct((32, 1024), F32),
            jax.ShapeDtypeStruct((16, 4, 1024), F32),
            jax.ShapeDtypeStruct((16, 512, 128), F32),
        ),
        in_specs=[tiles, any_, any_, any_, any_,
                  fixed((16, 4, 1024)), fixed((16, 4, 1024)), fixed((32, 1024))],
        out_specs=(
            pl.BlockSpec((32, 1024), lambda b: (0, 0)),
            pl.BlockSpec((16, 4, 1024), lambda b: (0, 0, 0)),
            tiles,
        ),
        scratch_shapes=[
            pltpu.VMEM((2, 4, 128, 1024), F32),
            pltpu.VMEM((2, 4, 128, 1024), F32),
            pltpu.VMEM((4, 128, 1024), F32),
            pltpu.VMEM((4, 128, 1024), F32),
            pltpu.VMEM((64, 1024), F32),
            pltpu.VMEM((2, 8, 1024, 128), F32),
            pltpu.VMEM((1024, 1024), BF16), pltpu.VMEM((1024, 1024), BF16),
            pltpu.VMEM((1024, 1024), BF16), pltpu.VMEM((1024, 1024), BF16),
            pltpu.VMEM((ROWS, 1024), BF16), pltpu.VMEM((ROWS, 1024), BF16),
            pltpu.VMEM((ROWS, 1024), BF16), pltpu.VMEM((ROWS, 1024), BF16),
            pltpu.VMEM((512, 1024), BF16), pltpu.VMEM((512, 1024), BF16),
            pltpu.SemaphoreType.DMA((22,)),
        ],
        compiler_params=pltpu.CompilerParams(
            dimension_semantics=("arbitrary",), vmem_limit_bytes=63 * 1024 * 1024
        ),
        name="update",
    )(trailing, g, cm, cp, hh, pown, fown, iown)


def body(inverse_factor, diag_block, panel_matrix, panel_factor, trailing):
    g, cm, cp, hh = gather(
        panel_matrix.reshape(4, 4, 4, 1024), panel_factor.reshape(4, 4, 4, 1024),
        inverse_factor, diag_block,
    )
    red, panel, out = update(
        g, cm, cp, hh,
        panel_matrix.reshape(16, 4, 1024), panel_factor.reshape(16, 4, 1024), inverse_factor,
        trailing.reshape(16, 512, 128),
    )
    return red, panel.reshape(panel_matrix.shape), out.reshape(trailing.shape)


def solution(mesh):
    rows = P(None, "prow", "pcol", None)
    tiles = P(None, "prow", None, None, "pcol", None)
    return jax.shard_map(
        body,
        mesh=mesh,
        in_specs=(P("pcol", None), P("pcol", None), rows, rows, tiles),
        out_specs=(P("pcol", None), rows, tiles),
        check_vma=False,
    )
```

```python
import functools

import jax
import jax.numpy as jnp
from jax import lax
from jax.experimental import pallas as pl
from jax.experimental.pallas import tpu as pltpu
from jax.sharding import PartitionSpec as P

MESH = pl.DeviceIdType.MESH
F32 = jnp.float32
BF16 = jnp.bfloat16


E_PASSES = (
    (4, ((0, 0),)),
    (5, ((1, 0), (0, 1), (0, 3))),
    (6, ((1, 3), (1, 1))),
    (7, ((0, 2), (1, 2))),
)


def comm_kernel(p_ref, f_ref, inv_ref, diag_ref, g_ref, cm_ref, cp_ref, h_ref,
                merged, swap, loc_sem, pre_send, pre_recv, xh_send, xh_recv,
                z_send, z_recv, d_send, d_recv, c_send, c_recv, cf_send, cd_send, cd_recv,
                xf_send, xf_recv, e_pre, ez_send, ez_recv, ey_send, ey_recv, ed_send, ed_recv):
    a = lax.axis_index("prow")
    c = lax.axis_index("pcol")
    xl, y = a // 4, a % 4
    z, xh, k = c // 4, (c // 2) % 2, c % 2
    d = c // 2

    partner = (a, c + 1 - 2 * k)
    z_next = (a, ((z + 1) % 8) * 4 + xh * 2 + k)
    z_prev = (a, ((z + 7) % 8) * 4 + xh * 2 + k)
    x_far = (a, z * 4 + (1 - xh) * 2 + k)
    x_near = ((1 - xl) * 4 + y, c)
    x_side = ((1 - xl) * 4 + y, z * 4 + (1 - xh) * 2 + k)
    y_next = (xl * 4 + (y + 1) % 4, c)
    y_prev = (xl * 4 + (y + 3) % 4, c)
    z_to = (z_next, z_prev)

    def remote(src, dst, send, recv, to):
        return pltpu.make_async_remote_copy(
            src_ref=src, dst_ref=dst, send_sem=send, recv_sem=recv, device_id=to, device_id_type=MESH
        )

    barrier = pltpu.get_barrier_semaphore()
    for to in (partner, z_next, z_prev, x_far, x_near, x_side, y_next, y_prev):
        pl.semaphore_signal(barrier, inc=1, device_id=to, device_id_type=MESH)
    pl.semaphore_wait(barrier, 8)

    def h_rows(which, block, start, size):
        return h_ref.at[which, block, pl.ds(pl.multiple_of(start, 32), size), :]

    def plane(h, t):
        return lax.rem(z + 8 - t, 8) if h == 0 else lax.rem(z + t, 8)

    def rows8(t, h, e):
        side = lax.rem(xh + e, 2)
        return pl.ds(pl.multiple_of(16 * plane(h, t) + 8 * side, 8), 8)

    lanes = pl.ds(pl.multiple_of(128 * a, 128), 128)
    pairs = ((p_ref, f_ref, inv_ref, diag_ref), (f_ref, p_ref, diag_ref, inv_ref))
    for me in range(2):
        @pl.when(k == me)
        def _():
            _, other, e_own, e_other = pairs[me]
            remote(
                e_other.at[:, lanes], h_rows(1 - me, a, 32 * c, 32), e_pre.at[0], e_pre.at[1], partner
            ).start()
            remote(other, swap, pre_send, pre_recv, partner).start()
            pltpu.make_async_copy(e_own.at[:, lanes], h_rows(me, a, 32 * c, 32), e_pre.at[2]).start()

    pre = remote(f_ref, swap, pre_send, pre_recv, partner)
    mine_e = pltpu.make_async_copy(inv_ref.at[:, lanes], h_rows(k, a, 32 * c, 32), e_pre.at[2])
    mine_e.wait()
    pre_e = remote(
        inv_ref.at[:, lanes], h_rows(k, a, 32 * (c + 1 - 2 * k), 32), e_pre.at[0], e_pre.at[1], partner
    )
    pre_e.wait_recv()
    far_e = remote(h_rows(k, a, 64 * d, 64), h_rows(k, a, 64 * d, 64), e_pre.at[3], e_pre.at[4], x_far)
    far_e.start()
    pre.wait_recv()
    merged[:, :, 0:4, :] = jnp.where(k == 0, p_ref[...], swap[...])
    merged[:, :, 4:8, :] = jnp.where(k == 0, swap[...], f_ref[...])

    def half(h):
        return merged.at[pl.ds(2 * h, 2)]

    def z_ref(h, t, e, j):
        return g_ref.at[k, 2 * h + j, pl.ds(0, 4 - e), rows8(t, h, e), :]

    for j in range(2):
        for h in range(2):
            remote(
                merged.at[2 * h + j], z_ref(h, 0, 0, j), z_send.at[0], z_recv.at[h, 0, j, 0], z_to[h]
            ).start()

    def far(h, e):
        ref = g_ref.at[k, pl.ds(2 * h, 2), :, rows8(0, h, e), :]
        return remote(half(h), ref, xh_send.at[h], xh_recv.at[h], x_far)

    def xf_copy(h, t, e):
        ref = g_ref.at[k, pl.ds(2 * h, 2), pl.ds(3, 1), rows8(t, h, e), :]
        return remote(ref, ref, xf_send, xf_recv.at[h, t], x_far)

    for h in range(2):
        far(h, 0).start()
    mine = [
        pltpu.make_async_copy(
            half(h), g_ref.at[k, pl.ds(2 * h, 2), :, rows8(0, h, 0), :], loc_sem.at[h]
        )
        for h in range(2)
    ]
    for h in range(2):
        mine[h].start()

    def z_copy(h, t, e, j):
        ref = z_ref(h, t, e, j)
        return remote(ref, ref, z_send.at[e], z_recv.at[h, e, j, t], z_to[h])

    def z_got(h, t, e, j):
        ref = z_ref(h, t, e, j)
        return remote(ref, ref, z_send.at[e], z_recv.at[h, e, j, t - 1], z_to[h])

    def d_copy(h, t, e, which=None):
        ref = g_ref.at[k if which is None else which, pl.ds(2 * h, 2), :, rows8(t, h, e), :]
        return remote(ref, ref, d_send, d_recv, partner)

    def e_rows(which, dx, dy, h, t):
        block = lax.rem(xl + dx, 2) * 4 + lax.rem(y + dy, 4)
        return h_rows(which, block, 128 * plane(h, t), 128)

    def ez_copy(h, t):
        ref = e_rows(k, 0, 0, h, t)
        return remote(ref, ref, ez_send.at[h, t], ez_recv.at[h, t], z_to[h])

    def ez_got(h, t):
        ref = e_rows(k, 0, 0, h, t)
        return remote(ref, ref, ez_send.at[h, t - 1], ez_recv.at[h, t - 1], z_to[h])

    e_hops = (
        (0, 0, x_near, 1, 0),
        (0, 0, y_next, 0, 3),
        (0, 0, y_prev, 0, 1),
        (1, 0, y_next, 1, 3),
        (1, 0, y_prev, 1, 1),
        (0, 1, y_prev, 0, 2),
        (1, 3, y_next, 1, 2),
    )

    def e_copy(out, h, t):
        dx, dy, to, rx, ry = e_hops[out]
        ref = e_rows(k, dx, dy, h, t)
        return remote(ref, ref, ey_send.at[out, t + 4 * h], ey_recv.at[4 * rx + ry, t + 4 * h], to)

    def e_got(dx, dy, h, t):
        ref = e_rows(k, dx, dy, h, t)
        return remote(ref, ref, ey_send.at[0, t + 4 * h], ey_recv.at[4 * dx + dy, t + 4 * h], partner)

    def blk(dx, dy):
        return lax.rem(xl + dx, 2) * 4 + lax.rem(y + dy, 4)

    def lower(dx, dy, h, t):
        return plane(h, t) >= blk(dx, dy)

    def valid(h, t):
        return jnp.logical_and(t >= h, t <= 4 - h)

    def e_take(out_got, outs, h, t):
        dx, dy = out_got

        @pl.when(lower(dx, dy, h, t))
        def _():
            e_got(dx, dy, h, t).wait_recv()
            for out in outs:
                e_copy(out, h, t).start()

    def e_step(s):
        for h in range(2):
            @pl.when(jnp.logical_and(s <= 4 - h, lower(0, 0, h, s)))
            def _():
                ez_got(h, s).wait_recv()

                @pl.when(s < 4 - h)
                def _():
                    ez_copy(h, s).start()

                for out in range(3):
                    e_copy(out, h, s).start()

            @pl.when(valid(h, s - 1))
            def _():
                t = jnp.maximum(s - 1, h)
                e_take((1, 0), (3, 4), h, t)
                e_take((0, 1), (5,), h, t)
                e_take((0, 3), (), h, t)

            @pl.when(valid(h, s - 2))
            def _():
                t = jnp.maximum(s - 2, h)
                e_take((1, 3), (6,), h, t)
                e_take((1, 1), (), h, t)

            @pl.when(valid(h, s - 3))
            def _():
                t = jnp.maximum(s - 3, h)
                e_take((0, 2), (), h, t)
                e_take((1, 2), (), h, t)

        for at, blocks in E_PASSES:
            @pl.when(s == at)
            def _():
                e_pass_all(blocks, lambda copy: copy.start())

    def e_piece(dx, dy, p, which):
        ref = h_rows(which, blk(dx, dy), 128 * p, 128)
        return remote(ref, ref, ed_send, ed_recv, partner)

    def e_pass_all(blocks, act, which=None):
        def piece(p, carry):
            for dx, dy in blocks:
                @pl.when(p >= blk(dx, dy))
                def _():
                    act(e_piece(dx, dy, p, k if which is None else which))

            return carry

        lax.fori_loop(0, 8, piece, 0)

    q = z // 2
    in_plane = xl == z % 2
    y_out = (2, 1)

    def place(m):
        return lax.rem(y - (2 * xh + m) + 4, 4)

    def c_copy(m, h, t, e, out, from_g=False):
        dst = cm_ref.at[m, pl.ds(2 * h, 2), rows8(t, h, e), :]
        src = g_ref.at[k, pl.ds(2 * h, 2), q, rows8(t, h, e), :] if from_g else dst
        to = (x_near, y_next, y_prev)[out]
        return remote(src, dst, c_send.at[m, out], c_recv.at[m, h, t, e], to)

    def cd_copy(m, h, t, e):
        src = cm_ref.at[m, pl.ds(2 * h, 2), rows8(t, h, e), :]
        dst = cp_ref.at[pl.ds(2 * h, 2), rows8(t, h, e), :]
        return remote(src, dst, cd_send, cd_recv, partner)

    def is_source(m):
        return jnp.logical_and(in_plane, place(m) == 0)

    def off_root(m):
        return jnp.logical_and(jnp.logical_not(in_plane), place(m) == 0)

    def relays(m):
        return place(m) == (3, 1)[m]

    def is_side(m):
        return jnp.logical_and(in_plane, y == 2 * (1 - xh) + m)

    def side_copy(m, t, e):
        src = g_ref.at[k, pl.ds(2, 2), q, rows8(t, 1, e), :]
        dst = cm_ref.at[m, pl.ds(2, 2), rows8(t, 1, e), :]
        return remote(src, dst, cf_send.at[m], c_recv.at[m, 1, t, 1 - e], x_side)

    def source_sends(t, e):
        for m in range(2):
            @pl.when(is_source(m))
            def _():
                for h in range(2):
                    for out in range(h, 3):
                        c_copy(m, h, t, e, out, True).start()

            @pl.when(is_side(m))
            def _():
                side_copy(m, t, e).start()

    def take_columns(t, slot, lag):
        for m in range(2):
            r = place(m)
            when = (
                jnp.logical_or(off_root(m), jnp.logical_and(in_plane, r % 2 == 1)),
                jnp.logical_or(
                    jnp.logical_and(in_plane, r == 2),
                    jnp.logical_and(jnp.logical_not(in_plane), r % 2 == 1),
                ),
                jnp.logical_and(jnp.logical_not(in_plane), r == 2),
            )[lag - 1]

            @pl.when(jnp.logical_and(when, t >= 0))
            def _():
                s = jnp.maximum(t, 0)
                for h in range(2):
                    e = jnp.where(in_plane, slot, 1 - slot) if h == 1 else slot
                    c_copy(m, h, s, e, 0).wait_recv()

                    @pl.when(r == 0)
                    def _():
                        for out in (1, 2):
                            c_copy(m, h, s, e, out).start()

                    @pl.when(relays(m))
                    def _():
                        c_copy(m, h, s, e, y_out[m]).start()

                    @pl.when(k != m)
                    def _():
                        cd_copy(m, h, s, e).start()

    def after(t, e):
        source_sends(t, e)
        for h in range(2):
            d_copy(h, t, e).start()

    mine[0].wait()
    mine[1].wait()
    df = d + 1 - 2 * xh
    remote(
        h_rows(k, a, 64 * df, 64), h_rows(k, a, 64 * df, 64), e_pre.at[3], e_pre.at[4], x_far
    ).wait_recv()
    @pl.when(lower(0, 0, 0, 0))
    def _():
        for h in range(2):
            ez_copy(h, 0).start()
        for out in range(3):
            e_copy(out, 0, 0).start()

    after(0, 0)

    def step(s, carry):
        for j in range(2):
            for h in range(2):
                z_got(h, s, 0, j).wait_recv()

                @pl.when(s < 7)
                def _():
                    z_copy(h, s, 0, j).start()

        for h in range(2):
            xf_copy(h, s, 0).start()

        after(s, 0)
        for lag in (1, 2, 3):
            take_columns(s - lag, 0, lag)
        e_step(s)
        t = s - 1
        for h in range(2):
            @pl.when(t == 0)
            def _():
                far(h, 1).wait_recv()

        for j in range(2):
            for h in range(2):
                @pl.when(t > 0)
                def _():
                    z_got(h, jnp.maximum(t, 1), 1, j).wait_recv()

                z_copy(h, t, 1, j).start()

        for h in range(2):
            @pl.when(t > 0)
            def _():
                xf_copy(h, t, 1).wait_recv()

        after(t, 1)
        for lag in (1, 2, 3):
            take_columns(t - lag, 1, lag)
        return carry

    lax.fori_loop(1, 8, step, 0)
    last = jnp.int32(7)
    for h in range(2):
        for j in range(2):
            z_got(h, last, 1, j).wait_recv()
        xf_copy(h, last, 1).wait_recv()
    after(last, 1)
    for lag in (1, 2, 3):
        for back in range(lag, -1, -1):
            if back < lag:
                take_columns(last - back, 0, lag)
            take_columns(last - back, 1, lag)

    pre_e.wait_send()
    pre.wait_send()
    far_e.wait_send()
    for h in range(2):
        far(h, 0).wait_send()
        for t in range(5 - h):
            if t < 4 - h:
                @pl.when(lower(0, 0, h, t))
                def _():
                    ez_copy(h, t).wait_send()

            if t >= h:
                for out in range(7):
                    @pl.when(lower(*e_hops[out][:2], h, t))
                    def _():
                        e_copy(out, h, t).wait_send()

    def sent(ref, sem):
        remote(ref, ref, sem, xh_recv.at[0], partner).wait_send()

    steps = pl.ds(0, 112)
    sent(g_ref.at[k, pl.ds(0, 2), :, steps, :], z_send.at[0])
    sent(g_ref.at[k, pl.ds(0, 2), pl.ds(0, 3), steps, :], z_send.at[1])
    sent(g_ref.at[k, pl.ds(0, 2), pl.ds(0, 1), steps, :], xf_send)
    for m in range(2):
        whole, part = cm_ref.at[m], cm_ref.at[m, pl.ds(0, 2)]

        @pl.when(is_side(m))
        def _():
            sent(part, cf_send.at[m])

        @pl.when(is_source(m))
        def _():
            sent(part, c_send.at[m, 0])

        @pl.when(place(m) == 0)
        def _():
            for out in (1, 2):
                sent(whole, c_send.at[m, out])

        @pl.when(relays(m))
        def _():
            sent(whole, c_send.at[m, y_out[m]])

        @pl.when(jnp.logical_not(is_source(m)))
        def _():
            @pl.when(k != m)
            def _():
                sent(cp_ref, cd_send)

            @pl.when(k == m)
            def _():
                remote(cp_ref, cp_ref, cd_send, cd_recv, partner).wait_recv()

    deep = pl.ds(0, 576)
    sent(h_ref.at[k, :, deep, :], ed_send)
    remote(h_ref.at[1 - k, :, deep, :], h_ref.at[1 - k, :, deep, :], ed_send, ed_recv, partner).wait_recv()
    sent(g_ref.at[k], d_send)
    remote(g_ref.at[1 - k], g_ref.at[1 - k], d_send, d_recv, partner).wait_recv()


def gather(p4, f4, inverse_factor, diag_block):
    dma = pltpu.SemaphoreType.DMA
    return pl.pallas_call(
        comm_kernel,
        out_shape=(
            jax.ShapeDtypeStruct((2, 4, 4, 128, 1024), F32),
            jax.ShapeDtypeStruct((2, 4, 128, 1024), F32),
            jax.ShapeDtypeStruct((4, 128, 1024), F32),
            jax.ShapeDtypeStruct((2, 8, 1024, 128), F32),
        ),
        in_specs=[pl.BlockSpec(memory_space=pltpu.VMEM)] * 4,
        out_specs=(pl.BlockSpec(memory_space=pl.ANY),) * 4,
        scratch_shapes=[
            pltpu.VMEM((4, 4, 8, 1024), F32),
            pltpu.VMEM((4, 4, 4, 1024), F32),
            dma((2,)), dma, dma, dma((2,)), dma((2,)),
            dma((2,)), dma((2, 2, 2, 7)),
            dma, dma,
            dma((2, 3)), dma((2, 2, 8, 2)), dma((2,)),
            dma, dma,
            dma, dma((2, 8)),
            dma((5,)),
            dma((2, 4)), dma((2, 4)),
            dma((7, 8)), dma((8, 8)),
            dma, dma,
        ],
        compiler_params=pltpu.CompilerParams(collective_id=0, has_side_effects=True),
        name="gather",
    )(p4, f4, inverse_factor, diag_block)


def split(v):
    hi = v.astype(BF16)
    return hi, (v - hi.astype(F32)).astype(BF16)


def dot3(x, y, contract):
    (xh, xlo), (yh, ylo) = x, y
    dims = (((1,), (contract,)), ((), ()))
    dot = functools.partial(lax.dot_general, dimension_numbers=dims, preferred_element_type=F32)
    return dot(xh, yh) + dot(xlo, yh) + dot(xh, ylo)


ROWS = 608


def update_kernel(tr, g_ref, cm_ref, cp_ref, h_ref, pown, fown, iown,
                  red_ref, panel_ref, out_ref,
                  pb, fb, pc, fc, po, hv, ih, il, dh, dl, uh, ul, th, tl, vh, vl, sems):
    b = pl.program_id(0)
    a = lax.axis_index("prow")
    c = lax.axis_index("pcol")
    z, xh, k = c // 4, (c // 2) % 2, c % 2
    source = a == (z % 2) * 4 + 2 * xh + k

    def stream(n):
        return [
            pltpu.make_async_copy(g_ref.at[w, n], (pb, fb)[w].at[n % 2], sems.at[2 + 2 * w + n % 2])
            for w in range(2)
        ]

    def slices(g):
        deep = pl.ds(128 * g, 1024 - 128 * g)
        return [
            pltpu.make_async_copy(h_ref.at[w, g, deep], hv.at[w, g, deep], sems.at[6 + 8 * w + g])
            for w in range(2)
        ]

    @pl.when(b == 0)
    def _():
        for g in range(8):
            for copy in slices(g):
                copy.start()

        @pl.when(source)
        def _():
            pltpu.make_async_copy(g_ref.at[0, :, z // 2], pc, sems.at[0]).start()
            pltpu.make_async_copy(g_ref.at[1, :, z // 2], fc, sems.at[1]).start()

        @pl.when(jnp.logical_not(source))
        def _():
            @pl.when(k == 0)
            def _():
                pltpu.make_async_copy(cm_ref.at[0], pc, sems.at[0]).start()
                pltpu.make_async_copy(cp_ref, fc, sems.at[1]).start()

            @pl.when(k == 1)
            def _():
                pltpu.make_async_copy(cp_ref, pc, sems.at[0]).start()
                pltpu.make_async_copy(cm_ref.at[1], fc, sems.at[1]).start()

        for n in range(2):
            for copy in stream(n):
                copy.start()
        for g in range(8):
            lanes = slice(128 * g, 128 * g + 128)
            deep = slice(128 * g, 1024)
            for copy in slices(g):
                copy.wait()
            hi, lo = split(hv[0, g, deep])
            ih[deep, lanes] = hi
            il[deep, lanes] = lo
            hi, lo = split(hv[1, g, deep])
            dh[deep, lanes] = hi
            dl[deep, lanes] = lo
            if g % 2 == 1:
                top = slice(128 * g - 128, 128 * g)
                ih[top, lanes] = jnp.zeros((128, 128), BF16)
                il[top, lanes] = jnp.zeros((128, 128), BF16)
            for r in range(g + 1, 8):
                rows = slice(128 * r, 128 * r + 128)
                hi, lo = split(hv[1, g, rows].T)
                dh[lanes, rows] = hi
                dl[lanes, rows] = lo
        pltpu.make_async_copy(cm_ref.at[0], pc, sems.at[0]).wait()
        pltpu.make_async_copy(cm_ref.at[0], fc, sems.at[1]).wait()

        hi, lo = split(fc[...].reshape(512, 1024))
        th[0:512] = hi
        tl[0:512] = lo
        for i in range(16):
            po[4 * i:4 * i + 4] = fown[i]
        hi, lo = split(po[...])
        th[512:576] = hi
        tl[512:576] = lo
        for i in range(16):
            po[4 * i:4 * i + 4] = pown[i]
        for n in range(4):
            cols = slice(256 * n, 256 * n + 256)
            deep = slice(256 * n, 1024)
            u = dot3(
                (th[0:576, deep], tl[0:576, deep]), (ih[deep, cols], il[deep, cols]), 0
            )
            hi, lo = split(u)
            uh[0:576, cols] = hi
            ul[0:576, cols] = lo
        hi, lo = split(iown[...])
        uh[576:608] = hi
        ul[576:608] = lo
        for n in range(4):
            cols = slice(256 * n, 256 * n + 256)
            start = jnp.concatenate(
                [pc[:, :, cols].reshape(512, 256), po[:, cols], jnp.zeros((32, 256), F32)]
            )
            t = start - dot3((uh[...], ul[...]), (dh[:, cols], dl[:, cols]), 0)
            hi, lo = split(t)
            th[:, cols] = hi
            tl[:, cols] = lo
        for n in range(4):
            cols = slice(256 * n, 256 * n + 256)
            deep = slice(0, 256 * n + 256)
            v = dot3((th[:, deep], tl[:, deep]), (ih[cols, deep], il[cols, deep]), 1)
            hi, lo = split(v[0:512])
            vh[:, cols] = hi
            vl[:, cols] = lo
            for i in range(16):
                panel_ref[i, :, cols] = v[512 + 4 * i:516 + 4 * i]
            red_ref[:, cols] = -v[576:608]

    for n in range(4):
        @pl.when(b == n)
        def _():
            if 0 < n < 3:
                for copy in stream(n + 1):
                    copy.start()
            for copy in stream(n):
                copy.wait()
            wide = slice(0, 128 * n + 128)
            for q in range(2):
                first = split(pb[n % 2, 2 * q:2 * q + 2].reshape(256, 1024))
                second = split(fb[n % 2, 2 * q:2 * q + 2].reshape(256, 1024))
                total = dot3(first, (uh[wide], ul[wide]), 1) + dot3(second, (vh[wide], vl[wide]), 1)
                for p in range(2):
                    i = 2 * q + p
                    lower = 8 * i + a >= c
                    for j in range(4):
                        at = pl.ds(j, 128, stride=4)
                        held = tr[i, at, :]
                        if j <= n:
                            new = held - total[128 * p:128 * p + 128, 128 * j:128 * j + 128]
                            held = jnp.where(lower, new, held) if j == n else new
                        out_ref[i, at, :] = held


def update(g, cm, cp, hh, pown, fown, iown, trailing):
    any_ = pl.BlockSpec(memory_space=pl.ANY)
    fixed = lambda shape: pl.BlockSpec(shape, lambda b: (0,) * len(shape), pipeline_mode=pl.Buffered(1))
    tiles = pl.BlockSpec((4, 512, 128), lambda b: (b, 0, 0))
    return pl.pallas_call(
        update_kernel,
        grid=(4,),
        out_shape=(
            jax.ShapeDtypeStruct((32, 1024), F32),
            jax.ShapeDtypeStruct((16, 4, 1024), F32),
            jax.ShapeDtypeStruct((16, 512, 128), F32),
        ),
        in_specs=[tiles, any_, any_, any_, any_,
                  fixed((16, 4, 1024)), fixed((16, 4, 1024)), fixed((32, 1024))],
        out_specs=(
            pl.BlockSpec((32, 1024), lambda b: (0, 0)),
            pl.BlockSpec((16, 4, 1024), lambda b: (0, 0, 0)),
            tiles,
        ),
        scratch_shapes=[
            pltpu.VMEM((2, 4, 128, 1024), F32),
            pltpu.VMEM((2, 4, 128, 1024), F32),
            pltpu.VMEM((4, 128, 1024), F32),
            pltpu.VMEM((4, 128, 1024), F32),
            pltpu.VMEM((64, 1024), F32),
            pltpu.VMEM((2, 8, 1024, 128), F32),
            pltpu.VMEM((1024, 1024), BF16), pltpu.VMEM((1024, 1024), BF16),
            pltpu.VMEM((1024, 1024), BF16), pltpu.VMEM((1024, 1024), BF16),
            pltpu.VMEM((ROWS, 1024), BF16), pltpu.VMEM((ROWS, 1024), BF16),
            pltpu.VMEM((ROWS, 1024), BF16), pltpu.VMEM((ROWS, 1024), BF16),
            pltpu.VMEM((512, 1024), BF16), pltpu.VMEM((512, 1024), BF16),
            pltpu.SemaphoreType.DMA((22,)),
        ],
        compiler_params=pltpu.CompilerParams(
            dimension_semantics=("arbitrary",), vmem_limit_bytes=63 * 1024 * 1024
        ),
        name="update",
    )(trailing, g, cm, cp, hh, pown, fown, iown)


def body(inverse_factor, diag_block, panel_matrix, panel_factor, trailing):
    g, cm, cp, hh = gather(
        panel_matrix.reshape(4, 4, 4, 1024), panel_factor.reshape(4, 4, 4, 1024),
        inverse_factor, diag_block,
    )
    red, panel, out = update(
        g, cm, cp, hh,
        panel_matrix.reshape(16, 4, 1024), panel_factor.reshape(16, 4, 1024), inverse_factor,
        trailing.reshape(16, 512, 128),
    )
    return red, panel.reshape(panel_matrix.shape), out.reshape(trailing.shape)


def solution(mesh):
    rows = P(None, "prow", "pcol", None)
    tiles = P(None, "prow", None, None, "pcol", None)
    return jax.shard_map(
        body,
        mesh=mesh,
        in_specs=(P("pcol", None), P("pcol", None), rows, rows, tiles),
        out_specs=(P("pcol", None), rows, tiles),
        check_vma=False,
    )
```
